32 devices in a mesh: term: 16 (over z, x, core), sector: 2 (over y).
Axes of the slice: x: 2, y: 2, z: 4, core: 2. Of those that a mesh axis runs over, the one named last changes fastest.
Arguments:
- wavefunction: bfloat16 [4, 512, 512], P('sector'), may hold values from -6 to 6
- left_operators: bfloat16 [256, 512, 512], P(('term', 'sector')), may hold values from -0.25 to 0.25
- right_operators: bfloat16 [256, 512, 512], P(('term', 'sector')), may hold values from -0.25 to 0.25
- source_sector: int32 [256], P(('term', 'sector')), may hold values from 0 to 3
- target_sector: int32 [256], P(('term', 'sector')), may hold values from 0 to 3
- live_terms: int32 [32], P(('term', 'sector')), may hold values from 1 to 8, as said below
- sector_rows: int32 [4], replicated, may hold values from 1 to 512, as said below
Outputs:
- sigma_blocks: float32 [4, 512, 512], P('sector', 'term')
The draws below stay inside these ranges and needn't reach their ends.
Inputs may be any that keep to these rules, and one draw needn't show every extreme that they name: Term group g = term index * 2 + sector index holds the term slots g * 8 to (g + 1) * 8 - 1; its live slots are the first live_terms[g]; some group has exactly 8. `sector_rows`: some sector uses exactly 512 rows.
All inputs are finite; a program needn't handle non-finite values.
Results may differ from the reference program's by a relative error of at most 0.0029.
Values may be sent and summed in bfloat16 or wider, within the bound.
A program may use at most 128 MiB of HBM per device.

```python
import jax
import jax.numpy as jnp
from jax import lax

R = 512
C = 512
TERM_DEV = 8
NSEC = 4
TERMS = 256
GROUPS = 32


def draw_live_terms(key, part):
    first = jax.random.fold_in(key, 11)
    second = jax.random.fold_in(key, 12)
    third = jax.random.fold_in(key, 13)
    small = jax.random.randint(first, (GROUPS,), 1, 3)
    heavy = jax.random.randint(second, (GROUPS,), 0, 16) == 0
    chosen = jax.random.randint(third, (), 0, GROUPS)
    heavy = heavy | (jnp.arange(GROUPS, dtype=jnp.int32) == chosen)
    return jnp.where(heavy, TERM_DEV, small).astype(jnp.int32)


def draw_sector_rows(key, part):
    first = jax.random.fold_in(key, 21)
    second = jax.random.fold_in(key, 22)
    third = jax.random.fold_in(key, 23)
    fourth = jax.random.fold_in(key, 24)
    fifth = jax.random.fold_in(key, 25)
    sizes_one = jax.random.randint(first, (NSEC,), 1, R + 1)
    sizes_two = jax.random.randint(second, (NSEC,), 1, R + 1)
    sizes = jnp.minimum(sizes_one, sizes_two)
    chosen = jax.random.randint(third, (), 0, NSEC)
    offset = jax.random.randint(fourth, (), 1, NSEC)
    partner = (chosen + offset) % NSEC
    partner_rows = jax.random.randint(fifth, (), R // 2, R)
    sector_ids = jnp.arange(NSEC, dtype=jnp.int32)
    sizes = jnp.where(sector_ids == partner, partner_rows, sizes)
    sizes = jnp.where(sector_ids == chosen, R, sizes)
    return sizes.astype(jnp.int32)


def set_ends(values, stream_key, smallest, high):
    longest = values.shape.index(max(values.shape))
    spots = []
    for shift in (0, 1):
        where = [jax.random.randint(jax.random.fold_in(stream_key, axis), (), 0, length) for axis, length in enumerate(values.shape)]
        where[longest] = (where[longest] + shift) % values.shape[longest]
        spots.append(tuple(where))
    return values.at[spots[0]].set(smallest).at[spots[1]].set(high)


def block_levels(stream_key, dims, pieces, low, largest):
    factor_of, own = 1.0, jax.random.fold_in(stream_key, 6)
    for position, blocks in pieces:
        steps = jnp.exp(jax.random.uniform(jax.random.fold_in(own, position), (blocks,), jnp.float32, low / len(pieces), largest / len(pieces)))
        factor_of = factor_of * jnp.repeat(steps, dims[position] // blocks).reshape([-1 if axis == position else 1 for axis in range(len(dims))])
    return factor_of


def normal_values(own_key, extent, deviation, reach, pieces=(), kind=jnp.bfloat16):
    result = jax.random.normal(own_key, extent, jnp.float32) * deviation
    if len(pieces) > 0:
        result = block_levels(own_key, extent, pieces, -0.22, 0.18) * result
    return jnp.clip(result, min=-reach, max=reach).astype(kind)


def setup_inputs(seed: int = 0) -> dict:
    key_of = jax.random.split(jax.random.key(seed), 8)
    wavefunction = normal_values(key_of[0], (NSEC, R, C), 1.0, 6.0, ((0, 2),))
    left_operators = normal_values(key_of[1], (TERMS, R, R), R ** -0.5, 0.25, ((0, 32),))
    right_operators = normal_values(key_of[2], (TERMS, C, C), C ** -0.5, 0.25, ((0, 32),))
    source_sector = set_ends(jax.random.randint(key_of[3], (TERMS,), 0, NSEC), jax.random.fold_in(key_of[3], 1), 0, NSEC - 1).astype(jnp.int32)
    target_sector = set_ends(jax.random.randint(key_of[4], (TERMS,), 0, NSEC), jax.random.fold_in(key_of[4], 1), 0, NSEC - 1).astype(jnp.int32)
    live_terms = draw_live_terms(jax.random.fold_in(key_of[7], 71), 0)
    sector_rows = draw_sector_rows(jax.random.fold_in(key_of[7], 71), 0)
    return dict(wavefunction=wavefunction, left_operators=left_operators, right_operators=right_operators, source_sector=source_sector, target_sector=target_sector, live_terms=live_terms, sector_rows=sector_rows)


def reference(wavefunction, left_operators, right_operators, source_sector, target_sector, live_terms, sector_rows):
    row_ids = jnp.arange(R, dtype=jnp.int32)
    slot_ids = jnp.arange(TERMS, dtype=jnp.int32)
    live_mask = (slot_ids % TERM_DEV) < live_terms[slot_ids // TERM_DEV]
    sigma = jnp.zeros((NSEC, R, C), jnp.float32)

    def apply_term(slot, partial_value):
        def contribute(partial_value):
            source_index = source_sector[slot].astype(jnp.int32)
            target_index = target_sector[slot].astype(jnp.int32)
            source = lax.dynamic_index_in_dim(wavefunction, source_index, 0, keepdims=False)
            keep_rows = (row_ids < sector_rows[source_index])[:, None]
            source = jnp.where(keep_rows, source, jnp.zeros_like(source))
            left_half = jnp.dot(left_operators[slot], source, preferred_element_type=jnp.float32).astype(jnp.bfloat16)
            product = lax.dot_general(left_half, right_operators[slot], (((1,), (1,)), ((), ())), preferred_element_type=jnp.float32)
            current = lax.dynamic_index_in_dim(partial_value, target_index, 0, keepdims=True)
            return lax.dynamic_update_index_in_dim(partial_value, current + product[None], target_index, 0)

        return lax.cond(live_mask[slot], contribute, lambda kept: kept, partial_value)

    sigma = lax.fori_loop(0, TERMS, apply_term, sigma)
    used = row_ids[None, :, None] < sector_rows[:, None, None]
    return jnp.where(used, sigma, jnp.zeros_like(sigma))
```

```python
import functools

import jax
import jax.numpy as jnp
from jax import lax
from jax.experimental import pallas as pl
from jax.experimental.pallas import tpu as pltpu
from jax.sharding import PartitionSpec as P

BF16 = jnp.bfloat16
F32 = jnp.float32
STEPS = 8
RELAYED = 6
LAG = 8


def kernel(
    dims,
    wave,
    left,
    right,
    source_ref,
    target_ref,
    live_hbm,
    rows_ref,
    out,
    near,
    far,
    lbuf,
    rbuf,
    half,
    prod,
    snd_c,
    rcv_c,
    acc,
    snd_a1,
    rcv_a1,
    snd_b1,
    rcv_b1,
    snd_a2,
    rcv_a2,
    snd_b2,
    rcv_b2,
    snd_z,
    rcv_z,
    live_ref,
    order,
    joins,
    upto,
    has,
    load_sem,
    ready,
    g_send,
    g_recv,
    e_send,
    e_recv,
    h_send,
    h_recv,
    f_send,
    f_recv,
    c_send,
    c_recv,
    sa1,
    ra1,
    sb1,
    rb1,
    sa2,
    ra2,
    sb2,
    rb2,
    sz,
    rz,
):
    Z, X, S, K, B, C = dims
    H, Q = C // 2, C // 4
    R = wave.shape[1]
    M = R // X
    slots = left.shape[0]
    term = lax.axis_index("term")
    ym = lax.axis_index("sector")
    cm = lax.rem(term, 2)
    xm = lax.rem(term // 2, X)
    zm = term // (2 * X)
    co = 1 - cm
    xo = 1 - xm

    def dev(z, x, c, y):
        return ((z * X + x) * 2 + c, y)

    core_peer = dev(zm, xm, co, ym)
    x_peer = dev(zm, xo, cm, ym)

    def y_other(d):
        return lax.rem(ym + d, S)

    def y_peer(d):
        return dev(zm, xm, cm, y_other(d))

    def z_other(d):
        if Z & (Z - 1):
            return lax.rem(zm + d, Z)
        other, bit = zm, 1
        while bit < Z:
            if d & bit:
                other = other + bit * (1 - 2 * lax.rem(zm // bit, 2))
            bit *= 2
        return other

    def z_peer(d):
        return dev(z_other(d), xm, cm, ym)

    def remote(src, dst, ssem, rsem, peer):
        return pltpu.make_async_remote_copy(
            src_ref=src,
            dst_ref=dst,
            send_sem=ssem,
            recv_sem=rsem,
            device_id=peer,
            device_id_type=pl.DeviceIdType.MESH,
        )

    def signal(sem, peer):
        pl.semaphore_signal(sem, inc=1, device_id=peer, device_id_type=pl.DeviceIdType.MESH)

    barrier = pltpu.get_barrier_semaphore()
    z_sides = jnp.where(zm > 0, 1, 0) + jnp.where(zm < Z - 1, 1, 0)

    def signal_sides(sem):
        @pl.when(zm > 0)
        def _():
            signal(sem, dev(zm - 1, xm, cm, ym))

        @pl.when(zm < Z - 1)
        def _():
            signal(sem, dev(zm + 1, xm, cm, ym))

    direct = [core_peer, x_peer] + [y_peer(d) for d in range(1, S)]
    for peer in direct:
        signal(barrier, peer)
    signal_sides(barrier)

    mine = pl.ds(ym * K, K)

    def cols(x):
        return pl.ds(pl.multiple_of(x * H, 128), H)

    own_loads = [
        pltpu.make_async_copy(wave.at[:, :, cols(x)], held.at[mine], load_sem.at[n])
        for n, (x, held) in enumerate(((xm, near), (xo, far)))
    ]
    live_load = pltpu.make_async_copy(live_hbm, live_ref, load_sem.at[2])
    l_loads = [
        pltpu.make_async_copy(left.at[:, :, x, c], lbuf.at[:, x, c], load_sem.at[3 + 2 * x + c])
        for x in range(X)
        for c in range(2)
    ]
    r_loads = [
        pltpu.make_async_copy(
            right.at[:, :, cols(x)], rbuf.at[:, :, n * H : (n + 1) * H], load_sem.at[7 + n]
        )
        for n, x in enumerate((xm, xo))
    ]
    for cp in own_loads + [live_load] + l_loads + r_loads:
        cp.start()

    targets = [target_ref[t] for t in range(slots)]
    ranks = []
    for t in range(slots):
        rank = jnp.int32(0)
        for u in range(slots):
            ahead = targets[u] <= targets[t] if u < t else targets[u] < targets[t]
            if u != t:
                rank = rank + jnp.where(ahead, 1, 0)
        ranks.append(rank)
    before = jnp.int32(-1)
    for n in range(slots):
        slot, target = jnp.int32(0), jnp.int32(0)
        for t in range(slots):
            slot = jnp.where(ranks[t] == n, t, slot)
            target = jnp.where(ranks[t] == n, targets[t], target)
        order[n] = slot
        joins[n] = jnp.where(target == before, 1.0, 0.0)
        before = target
    for s in range(S * K):
        last, below = jnp.int32(0), jnp.int32(0)
        for t in range(slots):
            last = last + jnp.where(targets[t] <= s, 1, 0)
            below = below + jnp.where(targets[t] < s, 1, 0)
        upto[s] = last
        has[s] = jnp.where(last > below, 1.0, 0.0)
    prod[0] = jnp.zeros(prod.shape[1:], F32)
    live_load.wait()

    for cp in own_loads:
        cp.wait()
    pl.semaphore_wait(barrier, len(direct) + z_sides)
    if Z > 2:
        signal_sides(ready.at[0])

    step = R // STEPS
    tail = (STEPS - RELAYED) * step
    pieces = [(d, k, j) for k in range(K) for j in range(RELAYED) for d in range(1, S)]
    tails = [(d, k) for k in range(K) for d in range(1, S)]
    sent = []

    def begin(*copies):
        for cp in copies:
            cp.start()
            sent.append(cp)

    def part(held, d, k, j, c):
        sector = lax.rem(ym + S - d, S) * K + k
        rows = pl.ds(RELAYED * step, tail) if j == RELAYED else pl.ds(j * step, step)
        return held.at[sector, rows, pl.ds(pl.multiple_of(c * Q, 128), Q)]

    def y_copy(d, k, j, source):
        ref = part(near, source, k, j, cm)
        return remote(ref, ref, g_send.at[d - 1, k, j], g_recv.at[d - 1, k, j], y_peer(d))

    def y_far(d, k, source):
        ref = part(far, source, k, RELAYED, cm)
        return remote(ref, ref, e_send.at[d - 1, k], e_recv.at[d - 1, k], y_peer(d))

    def x_copy(d, k, j):
        ref = part(near, d, k, j, cm)
        dst = part(far, d, k, j, cm)
        return remote(ref, dst, h_send.at[d - 1, k, j], h_recv.at[d - 1, k, j], x_peer)

    def core_copy(d, k, j, n, c):
        ref = part((near, far)[n], d, k, j, c)
        return remote(ref, ref, f_send.at[n, d - 1, k, j], f_recv.at[n, d - 1, k, j], core_peer)

    for d, k, j in pieces:
        begin(y_copy(d, k, j, 0))
    for d, k in tails:
        begin(y_copy(d, k, RELAYED, 0))
    for d, k in tails:
        begin(y_far(d, k, 0))

    depth_ids = lax.broadcasted_iota(jnp.int32, (1, R), 1)
    chunk = 4 if slots % 4 == 0 else slots

    def first(n_held, x, g):
        held = (near, far)[n_held]
        for n in range(g * chunk, (g + 1) * chunk):
            t = order[n]
            source = source_ref[t]
            limit = jnp.where(t < live_ref[0], rows_ref[source], 0)
            keep = jnp.where(depth_ids < limit, 1.0, 0.0).astype(BF16)
            lmat = lbuf[t, x].reshape(M, R) * keep
            value = jnp.dot(lmat, held[source], preferred_element_type=F32).astype(BF16)
            half[n, x, :, n_held * H : (n_held + 1) * H] = value

    def second(i, x):
        for n in range(slots):
            total = lax.dot_general(
                half[n, x],
                rbuf[order[n], i * H : (i + 1) * H],
                (((1,), (1,)), ((), ())),
                preferred_element_type=F32,
            )
            prod[n + 1] = total.reshape(prod.shape[1:]) + prod[n] * joins[n]

    def core_send(i, xi):
        return remote(
            snd_c.at[i, xi], rcv_c.at[i, xi], c_send.at[i, xi], c_recv.at[i, xi], core_peer
        )

    def spread(i, xi):
        @pl.loop(0, S * K)
        def _(s):
            y, k = s // K, s % K
            away = prod[upto[s], co] * has[s]
            kept = prod[upto[s], cm] * has[s]
            for n in range(2):
                piece = slice(n * Q, (n + 1) * Q)
                snd_c[i, xi, n, y, k] = away[:, piece].astype(BF16).reshape(Z, B, Q)
                acc[i, xi, n, y, k] = kept[:, piece].reshape(Z, B, Q)

        begin(core_send(i, xi))

    handled = []

    def relay_far(count):
        for d, k, j in pieces[len(handled) : len(handled) + count]:
            x_copy(d, k, j).wait_recv()
            begin(core_copy(d, k, j, 1, cm))
            handled.append((d, k, j))

    for n, (d, k, j) in enumerate(pieces):
        y_copy(d, k, j, d).wait_recv()
        begin(x_copy(d, k, j), core_copy(d, k, j, 0, cm))
        if n >= LAG:
            relay_far(1)
    for d, k in tails:
        y_copy(d, k, RELAYED, d).wait_recv()
        begin(core_copy(d, k, RELAYED, 0, cm))
        relay_far(1)
    if Z > 2:
        pl.semaphore_wait(ready.at[0], z_sides)
        if Z > 3:
            signal_sides(ready.at[1])
    for cp in l_loads + r_loads:
        cp.wait()
    for d, k, j in pieces + [(d, k, RELAYED) for d, k in tails]:
        core_copy(d, k, j, 0, co).wait_recv()
    groups = slots // chunk
    work = [(x, g) for x in (xo, xm) for g in range(groups)]
    left_over = len(pieces) - len(handled)
    for n, (x, g) in enumerate(work):
        first(0, x, g)
        if n + 1 < len(work):
            relay_far(-(-left_over // (len(work) - 1)))
    relay_far(len(pieces))
    for d, k in tails:
        y_far(d, k, d).wait_recv()
        begin(core_copy(d, k, RELAYED, 1, cm))
    for d, k, j in pieces + [(d, k, RELAYED) for d, k in tails]:
        core_copy(d, k, j, 1, co).wait_recv()

    def base(i, xi, n, y):
        return acc[i, xi, n, y] + rcv_c[i, xi, n, y].astype(F32)

    def a1_copy(i, y):
        return remote(snd_a1.at[i, y], rcv_a1.at[i, y], sa1.at[i, y], ra1.at[i, y], x_peer)

    def b1_copy(i, xi, d):
        at = (i, xi, d - 1)
        return remote(snd_b1.at[at], rcv_b1.at[at], sb1.at[at], rb1.at[at], y_peer(d))

    def a2_copy(i, d):
        at = (i, d - 1)
        return remote(snd_a2.at[at], rcv_a2.at[at], sa2.at[at], ra2.at[at], y_peer(d))

    def b2_copy(i):
        return remote(snd_b2.at[i], rcv_b2.at[i], sb2.at[i], rb2.at[i], x_peer)

    def z_copy(i, n, d):
        at = (i, n, d - 1)
        return remote(snd_z.at[at], rcv_z.at[at], sz.at[at], rz.at[at], z_peer(d))

    def stage_one_away(i):
        core_send(i, 0).wait_recv()
        for d in range(1, S):
            yo = y_other(d)
            snd_a1[i, yo] = base(i, 0, 0, yo).astype(BF16)
            begin(a1_copy(i, yo))
            snd_b1[i, 0, d - 1] = base(i, 0, 1, yo).astype(BF16)
            begin(b1_copy(i, 0, d))
        snd_a1[i, ym] = base(i, 0, 0, ym).astype(BF16)
        begin(a1_copy(i, ym))

    def stage_one_kept(i):
        core_send(i, 1).wait_recv()
        for d in range(1, S):
            yo = y_other(d)
            snd_b1[i, 1, d - 1] = base(i, 1, 1, yo).astype(BF16)
            begin(b1_copy(i, 1, d))

    def stage_two(i):
        for d in range(1, S):
            yo = y_other(d)
            a1_copy(i, yo).wait_recv()
            snd_a2[i, d - 1] = (base(i, 1, 0, yo) + rcv_a1[i, yo].astype(F32)).astype(BF16)
            begin(a2_copy(i, d))
        total = base(i, 0, 1, ym)
        for d in range(1, S):
            b1_copy(i, 0, d).wait_recv()
            total = total + rcv_b1[i, 0, d - 1].astype(F32)
        snd_b2[i] = total.astype(BF16)
        begin(b2_copy(i))

    def z_own(i, n, z):
        total = acc[i, 1, n, ym, :, z] + rcv_c[i, 1, n, ym, :, z].astype(F32)
        if n == 0:
            total = total + rcv_a1[i, ym, :, z].astype(F32)
            for d in range(1, S):
                total = total + rcv_a2[i, d - 1, :, z].astype(F32)
        else:
            for d in range(1, S):
                total = total + rcv_b1[i, 1, d - 1, :, z].astype(F32)
            total = total + rcv_b2[i, :, z].astype(F32)
        return total

    def stage_three(i):
        for n in range(2):
            if n == 0:
                a1_copy(i, ym).wait_recv()
                for d in range(1, S):
                    a2_copy(i, d).wait_recv()
            else:
                for d in range(1, S):
                    b1_copy(i, 1, d).wait_recv()
                b2_copy(i).wait_recv()
            for d in range(Z - 1, 0, -1):
                snd_z[i, n, d - 1] = z_own(i, n, z_other(d)).astype(BF16)
                begin(z_copy(i, n, d))

    def first_far(x):
        for g in range(groups):
            first(1, x, g)

    first_far(xo)
    second(0, xo)
    spread(0, 0)
    first_far(xm)
    stage_one_away(0)
    second(0, xm)
    spread(0, 1)
    second(1, xo)
    spread(1, 0)
    stage_one_kept(0)
    second(1, xm)
    spread(1, 1)
    stage_one_away(1)
    stage_one_kept(1)
    stage_two(0)
    for p in range(1, Z - 2):
        pl.semaphore_wait(ready.at[p], z_sides)
        if p + 1 < Z - 2:
            signal_sides(ready.at[p + 1])
    stage_two(1)
    stage_three(0)
    stage_three(1)

    ids = term * B + lax.broadcasted_iota(jnp.int32, (B, Q), 0)
    for i in range(2):
        for n in range(2):
            total = z_own(i, n, zm)
            for d in range(Z - 1, 0, -1):
                z_copy(i, n, d).wait_recv()
                total = total + rcv_z[i, n, d - 1].astype(F32)
            col = (2 * i + n) * Q
            for k in range(K):
                used = ids < rows_ref[ym * K + k]
                out[k, :, col : col + Q] = jnp.where(used, total[k], 0.0)

    for cp in sent:
        cp.wait_send()


def local(mesh_sizes, wave, left, right, source, target, live, sector_rows):
    T, S = mesh_sizes
    X = 2
    Z = T // (2 * X)
    K, R, C = wave.shape
    B = R // T
    H, Q = C // 2, C // 4
    slots = left.shape[0]
    dims = (Z, X, S, K, B, C)
    left = left.reshape(slots, Z, X, 2, B, R)
    vm = pltpu.VMEM
    dma = pltpu.SemaphoreType.DMA
    share = (K, Z, B, Q)
    scratch = [
        vm((S * K, R, H), BF16),
        vm((S * K, R, H), BF16),
        vm((slots, X, 2, Z, B, R), BF16),
        vm((slots, C, C), BF16),
        vm((slots, X, R // X, C), BF16),
        vm((slots + 1, 2, Z * B, H), F32),
        vm((2, 2, 2, S) + share, BF16),
        vm((2, 2, 2, S) + share, BF16),
        vm((2, 2, 2, S) + share, F32),
        vm((2, S) + share, BF16),
        vm((2, S) + share, BF16),
        vm((2, 2, S - 1) + share, BF16),
        vm((2, 2, S - 1) + share, BF16),
        vm((2, S - 1) + share, BF16),
        vm((2, S - 1) + share, BF16),
        vm((2,) + share, BF16),
        vm((2,) + share, BF16),
        vm((2, 2, Z - 1, K, B, Q), BF16),
        vm((2, 2, Z - 1, K, B, Q), BF16),
        pltpu.SMEM((1,), jnp.int32),
        pltpu.SMEM((slots,), jnp.int32),
        pltpu.SMEM((slots,), F32),
        pltpu.SMEM((S * K,), jnp.int32),
        pltpu.SMEM((S * K,), F32),
        dma((9,)),
        pltpu.SemaphoreType.REGULAR((max(Z - 2, 1),)),
        dma((S - 1, K, RELAYED + 1)),
        dma((S - 1, K, RELAYED + 1)),
        dma((S - 1, K)),
        dma((S - 1, K)),
        dma((S - 1, K, RELAYED)),
        dma((S - 1, K, RELAYED)),
        dma((2, S - 1, K, RELAYED + 1)),
        dma((2, S - 1, K, RELAYED + 1)),
        dma((2, 2)),
        dma((2, 2)),
        dma((2, S)),
        dma((2, S)),
        dma((2, 2, S - 1)),
        dma((2, 2, S - 1)),
        dma((2, S - 1)),
        dma((2, S - 1)),
        dma((2,)),
        dma((2,)),
        dma((2, 2, Z - 1)),
        dma((2, 2, Z - 1)),
    ]
    any_spec = pl.BlockSpec(memory_space=pl.ANY)
    smem = pl.BlockSpec(memory_space=pltpu.SMEM)
    return pl.pallas_call(
        functools.partial(kernel, dims),
        out_shape=jax.ShapeDtypeStruct((K, B, C), F32),
        in_specs=[any_spec] * 3 + [smem] * 2 + [any_spec, smem],
        out_specs=pl.BlockSpec(memory_space=pltpu.VMEM),
        scratch_shapes=scratch,
        compiler_params=pltpu.CompilerParams(
            collective_id=0, has_side_effects=True, vmem_limit_bytes=60 * 1024 * 1024
        ),
    )(wave, left, right, source, target, live, sector_rows)


def solution(mesh):
    in_specs = (
        P("sector", None, None),
        P(("term", "sector"), None, None),
        P(("term", "sector"), None, None),
        P(("term", "sector")),
        P(("term", "sector")),
        P(("term", "sector")),
        P(),
    )
    out_specs = P("sector", "term", None)
    sizes = (mesh.shape["term"], mesh.shape["sector"])
    return jax.shard_map(
        functools.partial(local, sizes),
        mesh=mesh,
        in_specs=in_specs,
        out_specs=out_specs,
        check_vma=False,
    )
```

```python
import functools

import jax
import jax.numpy as jnp
from jax import lax
from jax.experimental import pallas as pl
from jax.experimental.pallas import tpu as pltpu
from jax.sharding import PartitionSpec as P

BF16 = jnp.bfloat16
F32 = jnp.float32
STEPS = 8
RELAYED = 6
LAG = 7


def kernel(
    dims,
    wave,
    left,
    right,
    source_ref,
    target_ref,
    live_hbm,
    rows_ref,
    out,
    near,
    far,
    lbuf,
    rbuf,
    half,
    prod,
    snd_c,
    rcv_c,
    acc,
    snd_a1,
    rcv_a1,
    snd_b1,
    rcv_b1,
    snd_a2,
    rcv_a2,
    snd_b2,
    rcv_b2,
    snd_z,
    rcv_z,
    live_ref,
    order,
    joins,
    upto,
    has,
    load_sem,
    ready,
    g_send,
    g_recv,
    e_recv,
    h_recv,
    f_recv,
    r_send,
    c_recv,
    ra1,
    rb1,
    ra2,
    rb2,
    rz,
):
    Z, X, S, K, B, C = dims
    H, Q = C // 2, C // 4
    R = wave.shape[1]
    M = R // X
    slots = left.shape[0]
    term = lax.axis_index("term")
    ym = lax.axis_index("sector")
    cm = lax.rem(term, 2)
    xm = lax.rem(term // 2, X)
    zm = term // (2 * X)
    co = 1 - cm
    xo = 1 - xm

    def dev(z, x, c, y):
        return ((z * X + x) * 2 + c, y)

    core_peer = dev(zm, xm, co, ym)
    x_peer = dev(zm, xo, cm, ym)

    def y_other(d):
        return lax.rem(ym + d, S)

    def y_peer(d):
        return dev(zm, xm, cm, y_other(d))

    def z_other(d):
        if Z & (Z - 1):
            return lax.rem(zm + d, Z)
        other, bit = zm, 1
        while bit < Z:
            if d & bit:
                other = other + bit * (1 - 2 * lax.rem(zm // bit, 2))
            bit *= 2
        return other

    def z_peer(d):
        return dev(z_other(d), xm, cm, ym)

    def remote(src, dst, ssem, rsem, peer):
        return pltpu.make_async_remote_copy(
            src_ref=src,
            dst_ref=dst,
            send_sem=ssem,
            recv_sem=rsem,
            device_id=peer,
            device_id_type=pl.DeviceIdType.MESH,
        )

    def signal(sem, peer):
        pl.semaphore_signal(sem, inc=1, device_id=peer, device_id_type=pl.DeviceIdType.MESH)

    barrier = pltpu.get_barrier_semaphore()
    z_sides = jnp.where(zm > 0, 1, 0) + jnp.where(zm < Z - 1, 1, 0)

    def signal_sides(sem):
        @pl.when(zm > 0)
        def _():
            signal(sem, dev(zm - 1, xm, cm, ym))

        @pl.when(zm < Z - 1)
        def _():
            signal(sem, dev(zm + 1, xm, cm, ym))

    direct = [core_peer, x_peer] + [y_peer(d) for d in range(1, S)]
    for peer in direct:
        signal(barrier, peer)
    signal_sides(barrier)

    mine = pl.ds(ym * K, K)

    def cols(x):
        return pl.ds(pl.multiple_of(x * H, 128), H)

    own_loads = [
        pltpu.make_async_copy(wave.at[:, :, cols(x)], held.at[mine], load_sem.at[n])
        for n, (x, held) in enumerate(((xm, near), (xo, far)))
    ]
    live_load = pltpu.make_async_copy(live_hbm, live_ref, load_sem.at[2])
    l_loads = [
        pltpu.make_async_copy(left.at[:, :, x, c], lbuf.at[:, x, c], load_sem.at[3])
        for x in range(X)
        for c in range(2)
    ]
    r_loads = [
        pltpu.make_async_copy(
            right.at[:, :, cols(x)], rbuf.at[:, :, n * H : (n + 1) * H], load_sem.at[4]
        )
        for n, x in enumerate((xm, xo))
    ]
    for cp in own_loads + [live_load] + l_loads + r_loads:
        cp.start()

    targets = [target_ref[t] for t in range(slots)]
    ranks = []
    for t in range(slots):
        rank = jnp.int32(0)
        for u in range(slots):
            ahead = targets[u] <= targets[t] if u < t else targets[u] < targets[t]
            if u != t:
                rank = rank + jnp.where(ahead, 1, 0)
        ranks.append(rank)
    before = jnp.int32(-1)
    for n in range(slots):
        slot, target = jnp.int32(0), jnp.int32(0)
        for t in range(slots):
            slot = jnp.where(ranks[t] == n, t, slot)
            target = jnp.where(ranks[t] == n, targets[t], target)
        order[n] = slot
        joins[n] = jnp.where(target == before, 1.0, 0.0)
        before = target
    for s in range(S * K):
        last, below = jnp.int32(0), jnp.int32(0)
        for t in range(slots):
            last = last + jnp.where(targets[t] <= s, 1, 0)
            below = below + jnp.where(targets[t] < s, 1, 0)
        upto[s] = last
        has[s] = jnp.where(last > below, 1.0, 0.0)
    prod[0] = jnp.zeros(prod.shape[1:], F32)
    live_load.wait()

    for cp in own_loads:
        cp.wait()
    pl.semaphore_wait(barrier, len(direct) + z_sides)
    if Z > 2:
        signal_sides(ready.at[0])

    step = R // STEPS
    tail = (STEPS - RELAYED) * step
    pieces = [(d, k, j) for k in range(K) for j in range(RELAYED) for d in range(1, S)]
    tails = [(d, k) for k in range(K) for d in range(1, S)]

    def begin(*copies):
        for cp in copies:
            cp.start()

    def part(held, d, k, j, c):
        sector = lax.rem(ym + S - d, S) * K + k
        rows = pl.ds(RELAYED * step, tail) if j == RELAYED else pl.ds(j * step, step)
        return held.at[sector, rows, pl.ds(pl.multiple_of(c * Q, 128), Q)]

    def y_copy(d, k, j, source):
        ref = part(near, source, k, j, cm)
        return remote(ref, ref, g_send.at[0], g_recv.at[d - 1, k, j], y_peer(d))

    def y_far(d, k, source):
        ref = part(far, source, k, RELAYED, cm)
        return remote(ref, ref, g_send.at[1], e_recv.at[d - 1, k], y_peer(d))

    def x_copy(d, k, j):
        ref = part(near, d, k, j, cm)
        dst = part(far, d, k, j, cm)
        return remote(ref, dst, g_send.at[2], h_recv.at[d - 1, k, j], x_peer)

    def core_copy(d, k, j, n, c):
        ref = part((near, far)[n], d, k, j, c)
        return remote(ref, ref, g_send.at[3 + n], f_recv.at[n], core_peer)

    for d, k, j in pieces:
        begin(y_copy(d, k, j, 0))
    for d, k in tails:
        begin(y_copy(d, k, RELAYED, 0))
    for d, k in tails:
        begin(y_far(d, k, 0))

    depth_ids = lax.broadcasted_iota(jnp.int32, (1, R), 1)
    chunk = 4 if slots % 4 == 0 else slots

    def first(n_held, x, g):
        held = (near, far)[n_held]
        for n in range(g * chunk, (g + 1) * chunk):
            t = order[n]
            source = source_ref[t]
            limit = jnp.where(t < live_ref[0], rows_ref[source], 0)
            keep = jnp.where(depth_ids < limit, 1.0, 0.0).astype(BF16)
            lmat = lbuf[t, x].reshape(M, R) * keep
            value = jnp.dot(lmat, held[source], preferred_element_type=F32).astype(BF16)
            half[n, x, :, n_held * H : (n_held + 1) * H] = value

    def second(i, x):
        for n in range(slots):
            total = lax.dot_general(
                half[n, x],
                rbuf[order[n], i * H : (i + 1) * H],
                (((1,), (1,)), ((), ())),
                preferred_element_type=F32,
            )
            prod[n + 1] = total.reshape(prod.shape[1:]) + prod[n] * joins[n]

    def core_send(i, xi):
        return remote(
            snd_c.at[i, xi], rcv_c.at[i, xi], r_send.at[0], c_recv.at[i, xi], core_peer
        )

    def spread(i, xi):
        @pl.loop(0, S * K)
        def _(s):
            y, k = s // K, s % K
            away = prod[upto[s], co] * has[s]
            kept = prod[upto[s], cm] * has[s]
            for n in range(2):
                piece = slice(n * Q, (n + 1) * Q)
                snd_c[i, xi, n, y, k] = away[:, piece].astype(BF16).reshape(Z, B, Q)
                acc[i, xi, n, y, k] = kept[:, piece].reshape(Z, B, Q)

        begin(core_send(i, xi))

    handled = []

    def relay_far(count):
        for d, k, j in pieces[len(handled) : len(handled) + count]:
            x_copy(d, k, j).wait_recv()
            begin(core_copy(d, k, j, 1, cm))
            handled.append((d, k, j))

    for n, (d, k, j) in enumerate(pieces):
        y_copy(d, k, j, d).wait_recv()
        begin(x_copy(d, k, j), core_copy(d, k, j, 0, cm))
        if n >= LAG:
            relay_far(1)
    for d, k in tails:
        y_copy(d, k, RELAYED, d).wait_recv()
        begin(core_copy(d, k, RELAYED, 0, cm))
        relay_far(1)
    if Z > 2:
        pl.semaphore_wait(ready.at[0], z_sides)
        if Z > 3:
            signal_sides(ready.at[1])
    relay_far(len(pieces))
    for d, k in tails:
        y_far(d, k, d).wait_recv()
        begin(core_copy(d, k, RELAYED, 1, cm))
    pltpu.make_async_copy(lbuf, lbuf, load_sem.at[3]).wait()
    pltpu.make_async_copy(rbuf, rbuf, load_sem.at[4]).wait()
    others = pl.ds(0, (S - 1) * K)

    def shares(held, rows):
        return held.at[others, rows, pl.ds(0, Q)]

    whole, most, rest = pl.ds(0, R), pl.ds(0, RELAYED * step), pl.ds(0, tail)

    def all_of(held, rows, ssem, rsem, peer):
        return remote(shares(held, rows), shares(held, rows), ssem, rsem, peer)

    def base(i, xi, n, y):
        return acc[i, xi, n, y] + rcv_c[i, xi, n, y].astype(F32)

    def a1_copy(i, y):
        return remote(snd_a1.at[i, y], rcv_a1.at[i, y], r_send.at[1], ra1.at[i, y], x_peer)

    def b1_copy(i, xi, d):
        at = (i, xi, d - 1)
        return remote(snd_b1.at[at], rcv_b1.at[at], r_send.at[2], rb1.at[at], y_peer(d))

    def a2_copy(i, d, k):
        at = (i, d - 1, k)
        return remote(snd_a2.at[at], rcv_a2.at[at], r_send.at[3], ra2.at[at], y_peer(d))

    def b2_copy(i, k):
        at = (i, k)
        return remote(snd_b2.at[at], rcv_b2.at[at], r_send.at[4], rb2.at[at], x_peer)

    def z_copy(i, n, k, d):
        at = (i, n, k, d - 1)
        return remote(snd_z.at[at], rcv_z.at[at], r_send.at[5], rz.at[i, n, k], z_peer(d))

    def stage_one_away(i):
        core_send(i, 0).wait_recv()
        for d in range(1, S):
            yo = y_other(d)
            snd_a1[i, yo] = base(i, 0, 0, yo).astype(BF16)
            begin(a1_copy(i, yo))
            snd_b1[i, 0, d - 1] = base(i, 0, 1, yo).astype(BF16)
            begin(b1_copy(i, 0, d))

    def stage_one_own(i):
        snd_a1[i, ym] = base(i, 0, 0, ym).astype(BF16)
        begin(a1_copy(i, ym))

    def stage_one_kept(i):
        core_send(i, 1).wait_recv()
        for d in range(1, S):
            yo = y_other(d)
            snd_b1[i, 1, d - 1] = base(i, 1, 1, yo).astype(BF16)
            begin(b1_copy(i, 1, d))

    def stage_two(i):
        for d in range(1, S):
            a1_copy(i, y_other(d)).wait_recv()
        for d in range(1, S):
            b1_copy(i, 0, d).wait_recv()
        for k in range(K):
            for d in range(1, S):
                yo = y_other(d)
                total = acc[i, 1, 0, yo, k] + rcv_c[i, 1, 0, yo, k].astype(F32)
                snd_a2[i, d - 1, k] = (total + rcv_a1[i, yo, k].astype(F32)).astype(BF16)
                begin(a2_copy(i, d, k))
            total = acc[i, 0, 1, ym, k] + rcv_c[i, 0, 1, ym, k].astype(F32)
            for d in range(1, S):
                total = total + rcv_b1[i, 0, d - 1, k].astype(F32)
            snd_b2[i, k] = total.astype(BF16)
            begin(b2_copy(i, k))

    def z_own(i, n, k, z):
        total = acc[i, 1, n, ym, k, z] + rcv_c[i, 1, n, ym, k, z].astype(F32)
        if n == 0:
            total = total + rcv_a1[i, ym, k, z].astype(F32)
            for d in range(1, S):
                total = total + rcv_a2[i, d - 1, k, z].astype(F32)
        else:
            for d in range(1, S):
                total = total + rcv_b1[i, 1, d - 1, k, z].astype(F32)
            total = total + rcv_b2[i, k, z].astype(F32)
        return total

    def stage_three(i):
        a1_copy(i, ym).wait_recv()
        for d in range(1, S):
            b1_copy(i, 1, d).wait_recv()
        for k in range(K):
            for n in range(2):
                if n == 0:
                    for d in range(1, S):
                        a2_copy(i, d, k).wait_recv()
                else:
                    b2_copy(i, k).wait_recv()
                for d in range(Z - 1, 0, -1):
                    snd_z[i, n, k, d - 1] = z_own(i, n, k, z_other(d)).astype(BF16)
                    begin(z_copy(i, n, k, d))

    def first_all(n_held, x):
        for g in range(slots // chunk):
            first(n_held, x, g)

    all_of(near, whole, g_send.at[3], f_recv.at[0], core_peer).wait_recv()
    first_all(0, xo)
    all_of(far, whole, g_send.at[4], f_recv.at[1], core_peer).wait_recv()
    first_all(1, xo)
    second(0, xo)
    spread(0, 0)
    first_all(0, xm)
    first_all(1, xm)
    stage_one_away(0)
    stage_one_own(0)
    second(0, xm)
    spread(0, 1)
    second(1, xo)
    spread(1, 0)
    stage_one_kept(0)
    second(1, xm)
    spread(1, 1)
    stage_one_away(1)
    stage_two(0)
    stage_one_own(1)
    stage_one_kept(1)
    for p in range(1, Z - 2):
        pl.semaphore_wait(ready.at[p], z_sides)
        if p + 1 < Z - 2:
            signal_sides(ready.at[p + 1])
    stage_two(1)
    stage_three(0)
    stage_three(1)

    ids = term * B + lax.broadcasted_iota(jnp.int32, (B, Q), 0)
    for i in range(2):
        for k in range(K):
            used = ids < rows_ref[ym * K + k]
            for n in range(2):
                total = z_own(i, n, k, zm)
                got = rcv_z.at[i, n, k]
                remote(got, got, r_send.at[5], rz.at[i, n, k], core_peer).wait_recv()
                for d in range(Z - 1, 0, -1):
                    total = total + rcv_z[i, n, k, d - 1].astype(F32)
                col = (2 * i + n) * Q
                out[k, :, col : col + Q] = jnp.where(used, total, 0.0)

    all_of(near, whole, g_send.at[0], f_recv.at[0], core_peer).wait_send()
    all_of(far, rest, g_send.at[1], f_recv.at[0], core_peer).wait_send()
    all_of(near, most, g_send.at[2], f_recv.at[0], core_peer).wait_send()
    all_of(near, whole, g_send.at[3], f_recv.at[0], core_peer).wait_send()
    all_of(far, whole, g_send.at[4], f_recv.at[0], core_peer).wait_send()
    for n, ref in enumerate((snd_c, snd_a1, snd_b1, snd_a2, snd_b2, snd_z)):
        remote(ref, ref, r_send.at[n], f_recv.at[0], core_peer).wait_send()


def local(mesh_sizes, wave, left, right, source, target, live, sector_rows):
    T, S = mesh_sizes
    X = 2
    Z = T // (2 * X)
    K, R, C = wave.shape
    B = R // T
    H, Q = C // 2, C // 4
    slots = left.shape[0]
    dims = (Z, X, S, K, B, C)
    left = left.reshape(slots, Z, X, 2, B, R)
    vm = pltpu.VMEM
    dma = pltpu.SemaphoreType.DMA
    share = (K, Z, B, Q)
    scratch = [
        vm((S * K, R, H), BF16),
        vm((S * K, R, H), BF16),
        vm((slots, X, 2, Z, B, R), BF16),
        vm((slots, C, C), BF16),
        vm((slots, X, R // X, C), BF16),
        vm((slots + 1, 2, Z * B, H), F32),
        vm((2, 2, 2, S) + share, BF16),
        vm((2, 2, 2, S) + share, BF16),
        vm((2, 2, 2, S) + share, F32),
        vm((2, S) + share, BF16),
        vm((2, S) + share, BF16),
        vm((2, 2, S - 1) + share, BF16),
        vm((2, 2, S - 1) + share, BF16),
        vm((2, S - 1) + share, BF16),
        vm((2, S - 1) + share, BF16),
        vm((2,) + share, BF16),
        vm((2,) + share, BF16),
        vm((2, 2, K, Z - 1, B, Q), BF16),
        vm((2, 2, K, Z - 1, B, Q), BF16),
        pltpu.SMEM((1,), jnp.int32),
        pltpu.SMEM((slots,), jnp.int32),
        pltpu.SMEM((slots,), F32),
        pltpu.SMEM((S * K,), jnp.int32),
        pltpu.SMEM((S * K,), F32),
        dma((5,)),
        pltpu.SemaphoreType.REGULAR((max(Z - 2, 1),)),
        dma((5,)),
        dma((S - 1, K, RELAYED + 1)),
        dma((S - 1, K)),
        dma((S - 1, K, RELAYED)),
        dma((2,)),
        dma((6,)),
        dma((2, 2)),
        dma((2, S)),
        dma((2, 2, S - 1)),
        dma((2, S - 1, K)),
        dma((2, K)),
        dma((2, 2, K)),
    ]
    any_spec = pl.BlockSpec(memory_space=pl.ANY)
    smem = pl.BlockSpec(memory_space=pltpu.SMEM)
    return pl.pallas_call(
        functools.partial(kernel, dims),
        out_shape=jax.ShapeDtypeStruct((K, B, C), F32),
        in_specs=[any_spec] * 3 + [smem] * 2 + [any_spec, smem],
        out_specs=pl.BlockSpec(memory_space=pltpu.VMEM),
        scratch_shapes=scratch,
        compiler_params=pltpu.CompilerParams(
            collective_id=0, has_side_effects=True, vmem_limit_bytes=60 * 1024 * 1024
        ),
    )(wave, left, right, source, target, live, sector_rows)


def solution(mesh):
    in_specs = (
        P("sector", None, None),
        P(("term", "sector"), None, None),
        P(("term", "sector"), None, None),
        P(("term", "sector")),
        P(("term", "sector")),
        P(("term", "sector")),
        P(),
    )
    out_specs = P("sector", "term", None)
    sizes = (mesh.shape["term"], mesh.shape["sector"])
    return jax.shard_map(
        functools.partial(local, sizes),
        mesh=mesh,
        in_specs=in_specs,
        out_specs=out_specs,
        check_vma=False,
    )
```

```python
import functools

import jax
import jax.numpy as jnp
from jax import lax
from jax.experimental import pallas as pl
from jax.experimental.pallas import tpu as pltpu
from jax.sharding import PartitionSpec as P

BF16 = jnp.bfloat16
F32 = jnp.float32
STEPS = 8
RELAYED = 5
LAG = 8


def kernel(
    dims,
    wave,
    left,
    right,
    packed,
    out,
    near,
    far,
    lbuf,
    rbuf,
    half,
    prod,
    snd_c,
    rcv_c,
    acc,
    snd_a1,
    rcv_a1,
    snd_b1,
    rcv_b1,
    snd_a2,
    rcv_a2,
    snd_b2,
    rcv_b2,
    snd_z,
    rcv_z,
    order,
    joins,
    upto,
    has,
    load_sem,
    ready,
    g_send,
    g_recv,
    e_recv,
    h_recv,
    f_recv,
    r_send,
    c_recv,
    ra1,
    rb1,
    ra2,
    rb2,
    rz,
):
    Z, X, S, K, B, C = dims
    H, Q = C // 2, C // 4
    R = wave.shape[1]
    M = R // X
    slots = left.shape[0]
    term = lax.axis_index("term")
    ym = lax.axis_index("sector")
    cm = lax.rem(term, 2)
    xm = lax.rem(term // 2, X)
    zm = term // (2 * X)
    co = 1 - cm
    xo = 1 - xm

    def dev(z, x, c, y):
        return ((z * X + x) * 2 + c, y)

    core_peer = dev(zm, xm, co, ym)
    x_peer = dev(zm, xo, cm, ym)

    def y_other(d):
        return lax.rem(ym + d, S)

    def y_peer(d):
        return dev(zm, xm, cm, y_other(d))

    def z_other(d):
        if Z & (Z - 1):
            return lax.rem(zm + d, Z)
        other, bit = zm, 1
        while bit < Z:
            if d & bit:
                other = other + bit * (1 - 2 * lax.rem(zm // bit, 2))
            bit *= 2
        return other

    def z_peer(d):
        return dev(z_other(d), xm, cm, ym)

    def remote(src, dst, ssem, rsem, peer):
        return pltpu.make_async_remote_copy(
            src_ref=src,
            dst_ref=dst,
            send_sem=ssem,
            recv_sem=rsem,
            device_id=peer,
            device_id_type=pl.DeviceIdType.MESH,
        )

    def signal(sem, peer):
        pl.semaphore_signal(sem, inc=1, device_id=peer, device_id_type=pl.DeviceIdType.MESH)

    barrier = pltpu.get_barrier_semaphore()
    z_sides = jnp.where(zm > 0, 1, 0) + jnp.where(zm < Z - 1, 1, 0)

    def signal_sides(sem):
        @pl.when(zm > 0)
        def _():
            signal(sem, dev(zm - 1, xm, cm, ym))

        @pl.when(zm < Z - 1)
        def _():
            signal(sem, dev(zm + 1, xm, cm, ym))

    direct = [core_peer, x_peer] + [y_peer(d) for d in range(1, S)]
    for peer in direct:
        signal(barrier, peer)
    signal_sides(barrier)

    mine = pl.ds(ym * K, K)

    def cols(x):
        return pl.ds(pl.multiple_of(x * H, 128), H)

    own_loads = [
        pltpu.make_async_copy(wave.at[:, :, cols(x)], held.at[mine], load_sem.at[n])
        for n, (x, held) in enumerate(((xm, near), (xo, far)))
    ]
    l_loads = [
        pltpu.make_async_copy(left.at[:, :, x, c], lbuf.at[:, x, c], load_sem.at[3])
        for x in range(X)
        for c in range(2)
    ]
    r_loads = [
        pltpu.make_async_copy(
            right.at[:, :, cols(x)], rbuf.at[:, :, n * H : (n + 1) * H], load_sem.at[4]
        )
        for n, x in enumerate((xm, xo))
    ]
    for cp in own_loads + l_loads + r_loads:
        cp.start()

    targets = [packed[slots + t] for t in range(slots)]
    ranks = []
    for t in range(slots):
        rank = jnp.int32(0)
        for u in range(slots):
            ahead = targets[u] <= targets[t] if u < t else targets[u] < targets[t]
            if u != t:
                rank = rank + jnp.where(ahead, 1, 0)
        ranks.append(rank)
    before = jnp.int32(-1)
    for n in range(slots):
        slot, target = jnp.int32(0), jnp.int32(0)
        for t in range(slots):
            slot = jnp.where(ranks[t] == n, t, slot)
            target = jnp.where(ranks[t] == n, targets[t], target)
        order[n] = slot
        joins[n] = jnp.where(target == before, 1.0, 0.0)
        before = target
    for s in range(S * K):
        last, below = jnp.int32(0), jnp.int32(0)
        for t in range(slots):
            last = last + jnp.where(targets[t] <= s, 1, 0)
            below = below + jnp.where(targets[t] < s, 1, 0)
        upto[s] = last
        has[s] = jnp.where(last > below, 1.0, 0.0)
    prod[0] = jnp.zeros(prod.shape[1:], F32)

    for cp in own_loads:
        cp.wait()
    pl.semaphore_wait(barrier, len(direct) + z_sides)
    if Z > 2:
        signal_sides(ready.at[0])

    step = R // STEPS
    tail = (STEPS - RELAYED) * step
    pieces = [(d, k, j) for k in range(K) for j in range(RELAYED) for d in range(1, S)]
    tails = [(d, k) for k in range(K) for d in range(1, S)]

    def begin(*copies):
        for cp in copies:
            cp.start()

    def part(held, d, k, j, c):
        sector = lax.rem(ym + S - d, S) * K + k
        rows = pl.ds(RELAYED * step, tail) if j == RELAYED else pl.ds(j * step, step)
        return held.at[sector, rows, pl.ds(pl.multiple_of(c * Q, 128), Q)]

    def y_copy(d, k, j, source):
        ref = part(near, source, k, j, cm)
        return remote(ref, ref, g_send.at[0], g_recv.at[d - 1, k, j], y_peer(d))

    def y_far(d, k, source):
        ref = part(far, source, k, RELAYED, cm)
        return remote(ref, ref, g_send.at[1], e_recv.at[d - 1, k], y_peer(d))

    def x_copy(d, k, j):
        ref = part(near, d, k, j, cm)
        dst = part(far, d, k, j, cm)
        return remote(ref, dst, g_send.at[2], h_recv.at[d - 1, k, j], x_peer)

    def core_copy(d, k, j, n, c):
        ref = part((near, far)[n], d, k, j, c)
        return remote(ref, ref, g_send.at[3 + n], f_recv.at[n], core_peer)

    for d, k, j in pieces:
        begin(y_copy(d, k, j, 0))
    for d, k in tails:
        begin(y_copy(d, k, RELAYED, 0))
    for d, k in tails:
        begin(y_far(d, k, 0))

    depth_ids = lax.broadcasted_iota(jnp.int32, (1, R), 1)
    chunk = 4 if slots % 4 == 0 else slots

    def first(n_held, x, g):
        held = (near, far)[n_held]
        for n in range(g * chunk, (g + 1) * chunk):
            t = order[n]
            source = packed[t]
            limit = jnp.where(t < packed[2 * slots], packed[2 * slots + 1 + source], 0)
            keep = jnp.where(depth_ids < limit, 1.0, 0.0).astype(BF16)
            lmat = lbuf[t, x].reshape(M, R) * keep
            value = jnp.dot(lmat, held[source], preferred_element_type=F32).astype(BF16)
            half[n, x, :, n_held * H : (n_held + 1) * H] = value

    def second(i, x):
        for n in range(slots):
            total = lax.dot_general(
                half[n, x],
                rbuf[order[n], i * H : (i + 1) * H],
                (((1,), (1,)), ((), ())),
                preferred_element_type=F32,
            )
            prod[n + 1] = total.reshape(prod.shape[1:]) + prod[n] * joins[n]

    def core_send(i, xi):
        return remote(
            snd_c.at[i, xi], rcv_c.at[i, xi], r_send.at[0], c_recv.at[i, xi], core_peer
        )

    def spread(i, xi):
        @pl.loop(0, S * K)
        def _(s):
            y, k = s // K, s % K
            away = prod[upto[s], co] * has[s]
            kept = prod[upto[s], cm] * has[s]
            for n in range(2):
                piece = slice(n * Q, (n + 1) * Q)
                snd_c[i, xi, n, y, k] = away[:, piece].astype(BF16).reshape(Z, B, Q)
                acc[i, xi, n, y, k] = kept[:, piece].reshape(Z, B, Q)

        begin(core_send(i, xi))

    handled = []

    def relay_far(count):
        for d, k, j in pieces[len(handled) : len(handled) + count]:
            x_copy(d, k, j).wait_recv()
            begin(core_copy(d, k, j, 1, cm))
            handled.append((d, k, j))

    for n, (d, k, j) in enumerate(pieces):
        y_copy(d, k, j, d).wait_recv()
        begin(x_copy(d, k, j), core_copy(d, k, j, 0, cm))
        if n >= LAG:
            relay_far(1)
    for d, k in tails:
        y_copy(d, k, RELAYED, d).wait_recv()
        begin(core_copy(d, k, RELAYED, 0, cm))
        relay_far(1)
    if Z > 2:
        pl.semaphore_wait(ready.at[0], z_sides)
        if Z > 3:
            signal_sides(ready.at[1])
    relay_far(len(pieces))
    for d, k in tails:
        y_far(d, k, d).wait_recv()
        begin(core_copy(d, k, RELAYED, 1, cm))
    pltpu.make_async_copy(lbuf, lbuf, load_sem.at[3]).wait()
    pltpu.make_async_copy(rbuf, rbuf, load_sem.at[4]).wait()
    others = pl.ds(0, (S - 1) * K)

    def shares(held, rows):
        return held.at[others, rows, pl.ds(0, Q)]

    whole, most, rest = pl.ds(0, R), pl.ds(0, RELAYED * step), pl.ds(0, tail)

    def all_of(held, rows, ssem, rsem, peer):
        return remote(shares(held, rows), shares(held, rows), ssem, rsem, peer)

    def base(i, xi, n, y):
        return acc[i, xi, n, y] + rcv_c[i, xi, n, y].astype(F32)

    def a1_copy(i, y):
        return remote(snd_a1.at[i, y], rcv_a1.at[i, y], r_send.at[1], ra1.at[i, y], x_peer)

    def b1_copy(i, xi, d):
        at = (i, xi, d - 1)
        return remote(snd_b1.at[at], rcv_b1.at[at], r_send.at[2], rb1.at[at], y_peer(d))

    def a2_copy(i, d, k):
        at = (i, d - 1, k)
        return remote(snd_a2.at[at], rcv_a2.at[at], r_send.at[3], ra2.at[at], y_peer(d))

    def b2_copy(i, k):
        at = (i, k)
        return remote(snd_b2.at[at], rcv_b2.at[at], r_send.at[4], rb2.at[at], x_peer)

    def z_copy(i, n, k, d):
        at = (i, n, k, d - 1)
        return remote(snd_z.at[at], rcv_z.at[at], r_send.at[5], rz.at[i, n, k], z_peer(d))

    def stage_one_away(i):
        core_send(i, 0).wait_recv()
        for d in range(1, S):
            yo = y_other(d)
            snd_a1[i, yo] = base(i, 0, 0, yo).astype(BF16)
            begin(a1_copy(i, yo))
            snd_b1[i, 0, d - 1] = base(i, 0, 1, yo).astype(BF16)
            begin(b1_copy(i, 0, d))

    def stage_one_own(i):
        snd_a1[i, ym] = base(i, 0, 0, ym).astype(BF16)
        begin(a1_copy(i, ym))

    def stage_one_kept(i):
        core_send(i, 1).wait_recv()
        for d in range(1, S):
            yo = y_other(d)
            snd_b1[i, 1, d - 1] = base(i, 1, 1, yo).astype(BF16)
            begin(b1_copy(i, 1, d))

    def stage_two(i):
        for d in range(1, S):
            a1_copy(i, y_other(d)).wait_recv()
        for d in range(1, S):
            b1_copy(i, 0, d).wait_recv()
        for k in range(K):
            for d in range(1, S):
                yo = y_other(d)
                total = acc[i, 1, 0, yo, k] + rcv_c[i, 1, 0, yo, k].astype(F32)
                snd_a2[i, d - 1, k] = (total + rcv_a1[i, yo, k].astype(F32)).astype(BF16)
                begin(a2_copy(i, d, k))
            total = acc[i, 0, 1, ym, k] + rcv_c[i, 0, 1, ym, k].astype(F32)
            for d in range(1, S):
                total = total + rcv_b1[i, 0, d - 1, k].astype(F32)
            snd_b2[i, k] = total.astype(BF16)
            begin(b2_copy(i, k))

    def z_own(i, n, k, z):
        total = acc[i, 1, n, ym, k, z] + rcv_c[i, 1, n, ym, k, z].astype(F32)
        if n == 0:
            total = total + rcv_a1[i, ym, k, z].astype(F32)
            for d in range(1, S):
                total = total + rcv_a2[i, d - 1, k, z].astype(F32)
        else:
            for d in range(1, S):
                total = total + rcv_b1[i, 1, d - 1, k, z].astype(F32)
            total = total + rcv_b2[i, k, z].astype(F32)
        return total

    def stage_three(i):
        a1_copy(i, ym).wait_recv()
        for d in range(1, S):
            b1_copy(i, 1, d).wait_recv()
        for k in range(K):
            for n in range(2):
                if n == 0:
                    for d in range(1, S):
                        a2_copy(i, d, k).wait_recv()
                else:
                    b2_copy(i, k).wait_recv()
                for d in range(Z - 1, 0, -1):
                    snd_z[i, n, k, d - 1] = z_own(i, n, k, z_other(d)).astype(BF16)
                    begin(z_copy(i, n, k, d))

    def first_all(n_held, x):
        for g in range(slots // chunk):
            first(n_held, x, g)

    all_of(near, whole, g_send.at[3], f_recv.at[0], core_peer).wait_recv()
    first_all(0, xo)
    all_of(far, whole, g_send.at[4], f_recv.at[1], core_peer).wait_recv()
    first_all(1, xo)
    second(0, xo)
    spread(0, 0)
    first_all(0, xm)
    first_all(1, xm)
    stage_one_away(0)
    stage_one_own(0)
    second(0, xm)
    spread(0, 1)
    second(1, xo)
    spread(1, 0)
    stage_one_kept(0)
    second(1, xm)
    spread(1, 1)
    stage_one_away(1)
    stage_two(0)
    stage_one_own(1)
    stage_one_kept(1)
    for p in range(1, Z - 2):
        pl.semaphore_wait(ready.at[p], z_sides)
        if p + 1 < Z - 2:
            signal_sides(ready.at[p + 1])
    stage_two(1)
    stage_three(0)
    stage_three(1)

    ids = term * B + lax.broadcasted_iota(jnp.int32, (B, Q), 0)
    for i in range(2):
        for k in range(K):
            used = ids < packed[2 * slots + 1 + ym * K + k]
            for n in range(2):
                total = z_own(i, n, k, zm)
                got = rcv_z.at[i, n, k]
                remote(got, got, r_send.at[5], rz.at[i, n, k], core_peer).wait_recv()
                for d in range(Z - 1, 0, -1):
                    total = total + rcv_z[i, n, k, d - 1].astype(F32)
                col = (2 * i + n) * Q
                out[k, :, col : col + Q] = jnp.where(used, total, 0.0)

    all_of(near, whole, g_send.at[0], f_recv.at[0], core_peer).wait_send()
    all_of(far, rest, g_send.at[1], f_recv.at[0], core_peer).wait_send()
    all_of(near, most, g_send.at[2], f_recv.at[0], core_peer).wait_send()
    all_of(near, whole, g_send.at[3], f_recv.at[0], core_peer).wait_send()
    all_of(far, whole, g_send.at[4], f_recv.at[0], core_peer).wait_send()
    for n, ref in enumerate((snd_c, snd_a1, snd_b1, snd_a2, snd_b2, snd_z)):
        remote(ref, ref, r_send.at[n], f_recv.at[0], core_peer).wait_send()


def local(mesh_sizes, wave, left, right, source, target, live, sector_rows):
    T, S = mesh_sizes
    X = 2
    Z = T // (2 * X)
    K, R, C = wave.shape
    B = R // T
    H, Q = C // 2, C // 4
    slots = left.shape[0]
    dims = (Z, X, S, K, B, C)
    left = left.reshape(slots, Z, X, 2, B, R)
    vm = pltpu.VMEM
    dma = pltpu.SemaphoreType.DMA
    share = (K, Z, B, Q)
    scratch = [
        vm((S * K, R, H), BF16),
        vm((S * K, R, H), BF16),
        vm((slots, X, 2, Z, B, R), BF16),
        vm((slots, C, C), BF16),
        vm((slots, X, R // X, C), BF16),
        vm((slots + 1, 2, Z * B, H), F32),
        vm((2, 2, 2, S) + share, BF16),
        vm((2, 2, 2, S) + share, BF16),
        vm((2, 2, 2, S) + share, F32),
        vm((2, S) + share, BF16),
        vm((2, S) + share, BF16),
        vm((2, 2, S - 1) + share, BF16),
        vm((2, 2, S - 1) + share, BF16),
        vm((2, S - 1) + share, BF16),
        vm((2, S - 1) + share, BF16),
        vm((2,) + share, BF16),
        vm((2,) + share, BF16),
        vm((2, 2, K, Z - 1, B, Q), BF16),
        vm((2, 2, K, Z - 1, B, Q), BF16),
        pltpu.SMEM((slots,), jnp.int32),
        pltpu.SMEM((slots,), F32),
        pltpu.SMEM((S * K,), jnp.int32),
        pltpu.SMEM((S * K,), F32),
        dma((5,)),
        pltpu.SemaphoreType.REGULAR((max(Z - 2, 1),)),
        dma((5,)),
        dma((S - 1, K, RELAYED + 1)),
        dma((S - 1, K)),
        dma((S - 1, K, RELAYED)),
        dma((2,)),
        dma((6,)),
        dma((2, 2)),
        dma((2, S)),
        dma((2, 2, S - 1)),
        dma((2, S - 1, K)),
        dma((2, K)),
        dma((2, 2, K)),
    ]
    any_spec = pl.BlockSpec(memory_space=pl.ANY)
    smem = pl.BlockSpec(memory_space=pltpu.SMEM)
    return pl.pallas_call(
        functools.partial(kernel, dims),
        out_shape=jax.ShapeDtypeStruct((K, B, C), F32),
        in_specs=[any_spec] * 3 + [smem],
        out_specs=pl.BlockSpec(memory_space=pltpu.VMEM),
        scratch_shapes=scratch,
        compiler_params=pltpu.CompilerParams(
            collective_id=0, has_side_effects=True, vmem_limit_bytes=54784 * 1024
        ),
    )(wave, left, right, jnp.concatenate([source, target, live, sector_rows]))


def solution(mesh):
    in_specs = (
        P("sector", None, None),
        P(("term", "sector"), None, None),
        P(("term", "sector"), None, None),
        P(("term", "sector")),
        P(("term", "sector")),
        P(("term", "sector")),
        P(),
    )
    out_specs = P("sector", "term", None)
    sizes = (mesh.shape["term"], mesh.shape["sector"])
    return jax.shard_map(
        functools.partial(local, sizes),
        mesh=mesh,
        in_specs=in_specs,
        out_specs=out_specs,
        check_vma=False,
    )
```

```python
import functools

import jax
import jax.numpy as jnp
from jax import lax
from jax.experimental import pallas as pl
from jax.experimental.pallas import tpu as pltpu
from jax.sharding import PartitionSpec as P

BF16 = jnp.bfloat16
F32 = jnp.float32
STEPS = 8
RELAYED = 5
LAG = 8


def kernel(
    dims,
    wave,
    left,
    right,
    packed,
    out,
    near,
    far,
    lbuf,
    rbuf,
    half,
    prod,
    snd_c,
    rcv_c,
    acc,
    snd_a1,
    rcv_a1,
    snd_b1,
    rcv_b1,
    snd_a2,
    rcv_a2,
    snd_b2,
    rcv_b2,
    snd_z,
    rcv_z,
    order,
    joins,
    upto,
    has,
    load_sem,
    ready,
    g_send,
    g_recv,
    e_recv,
    h_recv,
    f_recv,
    r_send,
    z_send,
    c_recv,
    ra1,
    rb1,
    ra2,
    rb2,
    rz,
):
    Z, X, S, K, B, C = dims
    H, Q = C // 2, C // 4
    R = wave.shape[1]
    M = R // 2
    Z2 = Z // 2
    slots = left.shape[0]
    term = lax.axis_index("term")
    ym = lax.axis_index("sector")
    cm = lax.rem(term, 2)
    xm = lax.rem(term // 2, X)
    zm = term // (2 * X)
    co = 1 - cm
    xo = 1 - xm

    def dev(z, x, c, y):
        return ((z * X + x) * 2 + c, y)

    core_peer = dev(zm, xm, co, ym)
    x_peer = dev(zm, xo, cm, ym)

    def y_other(d):
        return lax.rem(ym + d, S)

    def y_peer(d):
        return dev(zm, xm, cm, y_other(d))

    def z_other(d):
        if Z & (Z - 1):
            return lax.rem(zm + d, Z)
        other, bit = zm, 1
        while bit < Z:
            if d & bit:
                other = other + bit * (1 - 2 * lax.rem(zm // bit, 2))
            bit *= 2
        return other

    def z_peer(d):
        return dev(z_other(d), xm, cm, ym)

    def remote(src, dst, ssem, rsem, peer):
        return pltpu.make_async_remote_copy(
            src_ref=src,
            dst_ref=dst,
            send_sem=ssem,
            recv_sem=rsem,
            device_id=peer,
            device_id_type=pl.DeviceIdType.MESH,
        )

    def signal(sem, peer):
        pl.semaphore_signal(sem, inc=1, device_id=peer, device_id_type=pl.DeviceIdType.MESH)

    barrier = pltpu.get_barrier_semaphore()
    z_sides = jnp.where(zm > 0, 1, 0) + jnp.where(zm < Z - 1, 1, 0)

    def signal_sides(sem):
        @pl.when(zm > 0)
        def _():
            signal(sem, dev(zm - 1, xm, cm, ym))

        @pl.when(zm < Z - 1)
        def _():
            signal(sem, dev(zm + 1, xm, cm, ym))

    direct = [core_peer, x_peer] + [y_peer(d) for d in range(1, S)]
    for peer in direct:
        signal(barrier, peer)
    signal_sides(barrier)

    mine = pl.ds(ym * K, K)

    def cols(x):
        return pl.ds(pl.multiple_of(x * H, 128), H)

    own_loads = [
        pltpu.make_async_copy(wave.at[:, :, cols(x)], held.at[mine], load_sem.at[n])
        for n, (x, held) in enumerate(((xm, near), (xo, far)))
    ]
    l_loads = [
        pltpu.make_async_copy(left.at[:, zh, :, x, c], lbuf.at[:, zh, c, x], load_sem.at[3])
        for zh in range(2)
        for x in range(X)
        for c in range(2)
    ]
    r_loads = [
        pltpu.make_async_copy(
            right.at[:, :, cols(x)], rbuf.at[:, :, n * H : (n + 1) * H], load_sem.at[4]
        )
        for n, x in enumerate((xm, xo))
    ]
    for cp in own_loads + l_loads + r_loads:
        cp.start()

    targets = [packed[slots + t] for t in range(slots)]
    ranks = []
    for t in range(slots):
        rank = jnp.int32(0)
        for u in range(slots):
            ahead = targets[u] <= targets[t] if u < t else targets[u] < targets[t]
            if u != t:
                rank = rank + jnp.where(ahead, 1, 0)
        ranks.append(rank)
    before = jnp.int32(-1)
    for n in range(slots):
        slot, target = jnp.int32(0), jnp.int32(0)
        for t in range(slots):
            slot = jnp.where(ranks[t] == n, t, slot)
            target = jnp.where(ranks[t] == n, targets[t], target)
        order[n] = slot
        joins[n] = jnp.where(target == before, 1.0, 0.0)
        before = target
    for s in range(S * K):
        last, below = jnp.int32(0), jnp.int32(0)
        for t in range(slots):
            last = last + jnp.where(targets[t] <= s, 1, 0)
            below = below + jnp.where(targets[t] < s, 1, 0)
        upto[s] = last
        has[s] = jnp.where(last > below, 1.0, 0.0)
    prod[0] = jnp.zeros(prod.shape[1:], F32)

    for cp in own_loads:
        cp.wait()
    pl.semaphore_wait(barrier, len(direct) + z_sides)
    if Z > 2:
        signal_sides(ready.at[0])

    step = R // STEPS
    tail = (STEPS - RELAYED) * step
    pieces = [(d, k, j) for k in range(K) for j in range(RELAYED) for d in range(1, S)]
    tails = [(d, k) for k in range(K) for d in range(1, S)]

    def begin(*copies):
        for cp in copies:
            cp.start()

    def part(held, d, k, j, c):
        sector = lax.rem(ym + S - d, S) * K + k
        rows = pl.ds(RELAYED * step, tail) if j == RELAYED else pl.ds(j * step, step)
        return held.at[sector, rows, pl.ds(pl.multiple_of(c * Q, 128), Q)]

    def y_copy(d, k, j, source):
        ref = part(near, source, k, j, cm)
        return remote(ref, ref, g_send.at[0], g_recv.at[d - 1, k, j], y_peer(d))

    def y_far(d, k, source):
        ref = part(far, source, k, RELAYED, cm)
        return remote(ref, ref, g_send.at[1], e_recv.at[d - 1, k], y_peer(d))

    def x_copy(d, k, j):
        ref = part(near, d, k, j, cm)
        dst = part(far, d, k, j, cm)
        return remote(ref, dst, g_send.at[2], h_recv.at[d - 1, k, j], x_peer)

    def core_copy(d, k, j, n, c):
        ref = part((near, far)[n], d, k, j, c)
        return remote(ref, ref, g_send.at[3 + n], f_recv.at[n], core_peer)

    for d, k, j in pieces:
        begin(y_copy(d, k, j, 0))
    for d, k in tails:
        begin(y_copy(d, k, RELAYED, 0))
    for d, k in tails:
        begin(y_far(d, k, 0))

    depth_ids = lax.broadcasted_iota(jnp.int32, (1, R), 1)
    chunk = 4 if slots % 4 == 0 else slots

    def first(n_held, zh, g):
        held = (near, far)[n_held]
        for n in range(g * chunk, (g + 1) * chunk):
            t = order[n]
            source = packed[t]
            limit = jnp.where(t < packed[2 * slots], packed[2 * slots + 1 + source], 0)
            keep = jnp.where(depth_ids < limit, 1.0, 0.0).astype(BF16)
            lmat = lbuf[t, zh].reshape(M, R) * keep
            value = jnp.dot(lmat, held[source], preferred_element_type=F32).astype(BF16)
            half[n, zh, :, n_held * H : (n_held + 1) * H] = value

    def second(zh, w):
        for n in range(slots):
            total = lax.dot_general(
                half[n, zh],
                rbuf[order[n], w * H : (w + 1) * H],
                (((1,), (1,)), ((), ())),
                preferred_element_type=F32,
            )
            prod[n + 1] = total.reshape(prod.shape[1:]) + prod[n] * joins[n]

    def core_send(zh, w):
        return remote(
            snd_c.at[zh, w], rcv_c.at[zh, w], r_send.at[0], c_recv.at[zh, w], core_peer
        )

    def spread(zh, w):
        @pl.loop(0, S * K)
        def _(s):
            y, k = s // K, s % K
            away = prod[upto[s], co] * has[s]
            kept = prod[upto[s], cm] * has[s]
            snd_c[zh, w, y, k] = away.astype(BF16).reshape(X, Z2, B, H)
            acc[zh, w, y, k] = kept.reshape(X, Z2, B, H)

        begin(core_send(zh, w))

    handled = []

    def relay_far(count):
        for d, k, j in pieces[len(handled) : len(handled) + count]:
            x_copy(d, k, j).wait_recv()
            begin(core_copy(d, k, j, 1, cm))
            handled.append((d, k, j))

    for n, (d, k, j) in enumerate(pieces):
        y_copy(d, k, j, d).wait_recv()
        begin(x_copy(d, k, j), core_copy(d, k, j, 0, cm))
        if n >= LAG:
            relay_far(1)
    for d, k in tails:
        y_copy(d, k, RELAYED, d).wait_recv()
        begin(core_copy(d, k, RELAYED, 0, cm))
        relay_far(1)
    if Z > 2:
        pl.semaphore_wait(ready.at[0], z_sides)
        if Z > 3:
            signal_sides(ready.at[1])
    relay_far(len(pieces))
    for d, k in tails:
        y_far(d, k, d).wait_recv()
        begin(core_copy(d, k, RELAYED, 1, cm))
    pltpu.make_async_copy(lbuf, lbuf, load_sem.at[3]).wait()
    pltpu.make_async_copy(rbuf, rbuf, load_sem.at[4]).wait()
    others = pl.ds(0, (S - 1) * K)

    def shares(held, rows):
        return held.at[others, rows, pl.ds(0, Q)]

    whole, most, rest = pl.ds(0, R), pl.ds(0, RELAYED * step), pl.ds(0, tail)

    def all_of(held, rows, ssem, rsem, peer):
        return remote(shares(held, rows), shares(held, rows), ssem, rsem, peer)

    def base(zh, w, y, k, x):
        return acc[zh, w, y, k, x] + rcv_c[zh, w, y, k, x].astype(F32)

    def a1_copy(zh, y):
        at = (zh, y)
        return remote(snd_a1.at[at], rcv_a1.at[at], r_send.at[1], ra1.at[at], x_peer)

    def b1_copy(zh, away, d):
        at = (zh, away, d - 1)
        return remote(snd_b1.at[at], rcv_b1.at[at], r_send.at[2], rb1.at[at], y_peer(d))

    def a2_copy(zh, d, k):
        at = (zh, d - 1, k)
        return remote(snd_a2.at[at], rcv_a2.at[at], r_send.at[3], ra2.at[at], y_peer(d))

    def b2_copy(zh, k):
        at = (zh, k)
        return remote(snd_b2.at[at], rcv_b2.at[at], r_send.at[4], rb2.at[at], x_peer)

    def z_copy(zh, w, k, i):
        z = zh * Z2 + i
        slot = lax.rem(zm - z - 1 + 2 * Z, Z)
        return remote(
            snd_z.at[zh, w, k, i],
            rcv_z.at[w, k, slot],
            z_send.at[zh, w, k, i],
            rz.at[w, k],
            dev(z, xm, cm, ym),
        )

    def stage_one_a(zh):
        core_send(zh, 0).wait_recv()
        for d in list(range(1, S)) + [0]:
            y = y_other(d)
            for k in range(K):
                snd_a1[zh, y, k] = base(zh, 0, y, k, xo).astype(BF16)
            begin(a1_copy(zh, y))

    def stage_one_b(zh):
        core_send(zh, 1).wait_recv()
        for away, x in ((0, xo), (1, xm)):
            for d in range(1, S):
                for k in range(K):
                    snd_b1[zh, away, d - 1, k] = base(zh, 1, y_other(d), k, x).astype(BF16)
                begin(b1_copy(zh, away, d))

    def stage_two_a(zh):
        for d in range(1, S):
            yo = y_other(d)
            a1_copy(zh, yo).wait_recv()
            for k in range(K):
                total = base(zh, 0, yo, k, xm) + rcv_a1[zh, yo, k].astype(F32)
                snd_a2[zh, d - 1, k] = total.astype(BF16)
                begin(a2_copy(zh, d, k))

    def stage_two_b(zh):
        for d in range(1, S):
            b1_copy(zh, 0, d).wait_recv()
        for k in range(K):
            total = base(zh, 1, ym, k, xo)
            for d in range(1, S):
                total = total + rcv_b1[zh, 0, d - 1, k].astype(F32)
            snd_b2[zh, k] = total.astype(BF16)
            begin(b2_copy(zh, k))

    def z_own(zh, w, k, i):
        total = acc[zh, w, ym, k, xm, i] + rcv_c[zh, w, ym, k, xm, i].astype(F32)
        if w == 0:
            total = total + rcv_a1[zh, ym, k, i].astype(F32)
            for d in range(1, S):
                total = total + rcv_a2[zh, d - 1, k, i].astype(F32)
        else:
            for d in range(1, S):
                total = total + rcv_b1[zh, 1, d - 1, k, i].astype(F32)
            total = total + rcv_b2[zh, k, i].astype(F32)
        return total

    def stage_three(zh):
        a1_copy(zh, ym).wait_recv()
        for d in range(1, S):
            b1_copy(zh, 1, d).wait_recv()
        for k in range(K):
            for w in range(2):
                if w == 0:
                    for d in range(1, S):
                        a2_copy(zh, d, k).wait_recv()
                else:
                    b2_copy(zh, k).wait_recv()
                for i in range(Z2):
                    @pl.when(zm != zh * Z2 + i)
                    def _():
                        snd_z[zh, w, k, i] = z_own(zh, w, k, i).astype(BF16)
                        begin(z_copy(zh, w, k, i))

    def first_all(n_held, zh):
        for g in range(slots // chunk):
            first(n_held, zh, g)

    all_of(near, whole, g_send.at[3], f_recv.at[0], core_peer).wait_recv()
    first_all(0, 0)
    all_of(far, whole, g_send.at[4], f_recv.at[1], core_peer).wait_recv()
    first_all(1, 0)
    second(0, 0)
    spread(0, 0)
    second(0, 1)
    spread(0, 1)
    stage_one_a(0)
    first_all(0, 1)
    stage_one_b(0)
    first_all(1, 1)
    second(1, 0)
    spread(1, 0)
    second(1, 1)
    spread(1, 1)
    stage_two_a(0)
    stage_two_b(0)
    stage_one_a(1)
    stage_one_b(1)
    for p in range(1, Z - 2):
        pl.semaphore_wait(ready.at[p], z_sides)
        if p + 1 < Z - 2:
            signal_sides(ready.at[p + 1])
    stage_three(0)
    stage_two_a(1)
    stage_two_b(1)
    stage_three(1)

    ids = term * B + lax.broadcasted_iota(jnp.int32, (B, H), 0)
    my_half, my_place = zm // Z2, lax.rem(zm, Z2)
    for k in range(K):
        used = ids < packed[2 * slots + 1 + ym * K + k]
        for w in range(2):
            total = z_own(my_half, w, k, my_place)
            got = rcv_z.at[w, k]
            remote(got, got, r_send.at[0], rz.at[w, k], core_peer).wait_recv()
            for n in range(Z - 1):
                total = total + rcv_z[w, k, n].astype(F32)
            out[k, :, w * H : (w + 1) * H] = jnp.where(used, total, 0.0)

    all_of(near, whole, g_send.at[0], f_recv.at[0], core_peer).wait_send()
    all_of(far, rest, g_send.at[1], f_recv.at[0], core_peer).wait_send()
    all_of(near, most, g_send.at[2], f_recv.at[0], core_peer).wait_send()
    all_of(near, whole, g_send.at[3], f_recv.at[0], core_peer).wait_send()
    all_of(far, whole, g_send.at[4], f_recv.at[0], core_peer).wait_send()
    for n, ref in enumerate((snd_c, snd_a1, snd_b1, snd_a2, snd_b2)):
        remote(ref, ref, r_send.at[n], f_recv.at[0], core_peer).wait_send()
    for zh in range(2):
        for i in range(Z2):
            @pl.when(zm != zh * Z2 + i)
            def _():
                for w in range(2):
                    for k in range(K):
                        z_copy(zh, w, k, i).wait_send()


def local(mesh_sizes, wave, left, right, source, target, live, sector_rows):
    T, S = mesh_sizes
    X = 2
    Z = T // (2 * X)
    K, R, C = wave.shape
    B = R // T
    H, Q = C // 2, C // 4
    slots = left.shape[0]
    dims = (Z, X, S, K, B, C)
    left = left.reshape(slots, 2, Z // 2, X, 2, B, R)
    vm = pltpu.VMEM
    dma = pltpu.SemaphoreType.DMA
    Z2 = Z // 2
    share = (K, Z2, B, H)
    scratch = [
        vm((S * K, R, H), BF16),
        vm((S * K, R, H), BF16),
        vm((slots, 2, 2, X, Z2, B, R), BF16),
        vm((slots, C, C), BF16),
        vm((slots, 2, R // 2, C), BF16),
        vm((slots + 1, 2, X * Z2 * B, H), F32),
        vm((2, 2, S, K, X, Z2, B, H), BF16),
        vm((2, 2, S, K, X, Z2, B, H), BF16),
        vm((2, 2, S, K, X, Z2, B, H), F32),
        vm((2, S) + share, BF16),
        vm((2, S) + share, BF16),
        vm((2, 2, S - 1) + share, BF16),
        vm((2, 2, S - 1) + share, BF16),
        vm((2, S - 1) + share, BF16),
        vm((2, S - 1) + share, BF16),
        vm((2,) + share, BF16),
        vm((2,) + share, BF16),
        vm((2, 2) + share, BF16),
        vm((2, K, Z - 1, B, H), BF16),
        pltpu.SMEM((slots,), jnp.int32),
        pltpu.SMEM((slots,), F32),
        pltpu.SMEM((S * K,), jnp.int32),
        pltpu.SMEM((S * K,), F32),
        dma((5,)),
        pltpu.SemaphoreType.REGULAR((max(Z - 2, 1),)),
        dma((5,)),
        dma((S - 1, K, RELAYED + 1)),
        dma((S - 1, K)),
        dma((S - 1, K, RELAYED)),
        dma((2,)),
        dma((5,)),
        dma((2, 2, K, Z2)),
        dma((2, 2)),
        dma((2, S)),
        dma((2, 2, S - 1)),
        dma((2, S - 1, K)),
        dma((2, K)),
        dma((2, K)),
    ]
    any_spec = pl.BlockSpec(memory_space=pl.ANY)
    smem = pl.BlockSpec(memory_space=pltpu.SMEM)
    return pl.pallas_call(
        functools.partial(kernel, dims),
        out_shape=jax.ShapeDtypeStruct((K, B, C), F32),
        in_specs=[any_spec] * 3 + [smem],
        out_specs=pl.BlockSpec(memory_space=pltpu.VMEM),
        scratch_shapes=scratch,
        compiler_params=pltpu.CompilerParams(
            collective_id=0, has_side_effects=True, vmem_limit_bytes=54784 * 1024
        ),
    )(wave, left, right, jnp.concatenate([source, target, live, sector_rows]))


def solution(mesh):
    in_specs = (
        P("sector", None, None),
        P(("term", "sector"), None, None),
        P(("term", "sector"), None, None),
        P(("term", "sector")),
        P(("term", "sector")),
        P(("term", "sector")),
        P(),
    )
    out_specs = P("sector", "term", None)
    sizes = (mesh.shape["term"], mesh.shape["sector"])
    return jax.shard_map(
        functools.partial(local, sizes),
        mesh=mesh,
        in_specs=in_specs,
        out_specs=out_specs,
        check_vma=False,
    )
```

```python
import functools

import jax
import jax.numpy as jnp
from jax import lax
from jax.experimental import pallas as pl
from jax.experimental.pallas import tpu as pltpu
from jax.sharding import PartitionSpec as P

BF16 = jnp.bfloat16
F32 = jnp.float32
STEPS = 8
RELAYED = 5
LAG = 8


def kernel(
    dims,
    wave,
    left,
    right,
    packed,
    out,
    near,
    far,
    lbuf,
    rbuf,
    half,
    prod,
    snd_c,
    rcv_c,
    snd_a1,
    rcv_a1,
    snd_b1,
    rcv_b1,
    snd_a2,
    rcv_a2,
    snd_b2,
    rcv_b2,
    snd_z,
    rcv_z,
    order,
    joins,
    upto,
    has,
    load_sem,
    ready,
    g_send,
    g_recv,
    e_recv,
    h_recv,
    f_recv,
    r_send,
    z_send,
    c_recv,
    ra1,
    rb1,
    ra2,
    rb2,
    rz,
):
    Z, X, S, K, B, C = dims
    H, Q = C // 2, C // 4
    R = wave.shape[1]
    M = R // 2
    Z2 = Z // 2
    slots = left.shape[0]
    term = lax.axis_index("term")
    ym = lax.axis_index("sector")
    cm = lax.rem(term, 2)
    xm = lax.rem(term // 2, X)
    zm = term // (2 * X)
    co = 1 - cm
    xo = 1 - xm

    def dev(z, x, c, y):
        return ((z * X + x) * 2 + c, y)

    core_peer = dev(zm, xm, co, ym)
    x_peer = dev(zm, xo, cm, ym)

    def y_other(d):
        return lax.rem(ym + d, S)

    def y_peer(d):
        return dev(zm, xm, cm, y_other(d))

    def z_other(d):
        if Z & (Z - 1):
            return lax.rem(zm + d, Z)
        other, bit = zm, 1
        while bit < Z:
            if d & bit:
                other = other + bit * (1 - 2 * lax.rem(zm // bit, 2))
            bit *= 2
        return other

    def z_peer(d):
        return dev(z_other(d), xm, cm, ym)

    def remote(src, dst, ssem, rsem, peer):
        return pltpu.make_async_remote_copy(
            src_ref=src,
            dst_ref=dst,
            send_sem=ssem,
            recv_sem=rsem,
            device_id=peer,
            device_id_type=pl.DeviceIdType.MESH,
        )

    def signal(sem, peer):
        pl.semaphore_signal(sem, inc=1, device_id=peer, device_id_type=pl.DeviceIdType.MESH)

    barrier = pltpu.get_barrier_semaphore()
    z_sides = jnp.where(zm > 0, 1, 0) + jnp.where(zm < Z - 1, 1, 0)

    def signal_sides(sem):
        @pl.when(zm > 0)
        def _():
            signal(sem, dev(zm - 1, xm, cm, ym))

        @pl.when(zm < Z - 1)
        def _():
            signal(sem, dev(zm + 1, xm, cm, ym))

    direct = [core_peer, x_peer] + [y_peer(d) for d in range(1, S)]
    for peer in direct:
        signal(barrier, peer)
    signal_sides(barrier)

    mine = pl.ds(ym * K, K)

    def cols(x):
        return pl.ds(pl.multiple_of(x * H, 128), H)

    own_loads = [
        pltpu.make_async_copy(wave.at[:, :, cols(x)], held.at[mine], load_sem.at[n])
        for n, (x, held) in enumerate(((xm, near), (xo, far)))
    ]
    l_loads = [
        pltpu.make_async_copy(left.at[:, zh, :, x, c], lbuf.at[:, zh, c, x], load_sem.at[3])
        for zh in range(2)
        for x in range(X)
        for c in range(2)
    ]
    r_loads = [
        pltpu.make_async_copy(
            right.at[:, :, cols(x)], rbuf.at[:, :, n * H : (n + 1) * H], load_sem.at[4]
        )
        for n, x in enumerate((xm, xo))
    ]
    for cp in own_loads + l_loads + r_loads:
        cp.start()

    targets = [packed[slots + t] for t in range(slots)]
    ranks = []
    for t in range(slots):
        rank = jnp.int32(0)
        for u in range(slots):
            ahead = targets[u] <= targets[t] if u < t else targets[u] < targets[t]
            if u != t:
                rank = rank + jnp.where(ahead, 1, 0)
        ranks.append(rank)
    before = jnp.int32(-1)
    for n in range(slots):
        slot, target = jnp.int32(0), jnp.int32(0)
        for t in range(slots):
            slot = jnp.where(ranks[t] == n, t, slot)
            target = jnp.where(ranks[t] == n, targets[t], target)
        order[n] = slot
        joins[n] = jnp.where(target == before, 1.0, 0.0)
        before = target
    for s in range(S * K):
        last, below = jnp.int32(0), jnp.int32(0)
        for t in range(slots):
            last = last + jnp.where(targets[t] <= s, 1, 0)
            below = below + jnp.where(targets[t] < s, 1, 0)
        upto[s] = jnp.maximum(last - 1, 0)
        has[s] = jnp.where(last > below, 1.0, 0.0)

    for cp in own_loads:
        cp.wait()
    pl.semaphore_wait(barrier, len(direct) + z_sides)
    if Z > 2:
        signal_sides(ready.at[0])

    step = R // STEPS
    tail = (STEPS - RELAYED) * step
    pieces = [(d, k, j) for k in range(K) for j in range(RELAYED) for d in range(1, S)]
    tails = [(d, k) for k in range(K) for d in range(1, S)]

    def begin(*copies):
        for cp in copies:
            cp.start()

    def part(held, d, k, j, c):
        sector = lax.rem(ym + S - d, S) * K + k
        rows = pl.ds(RELAYED * step, tail) if j == RELAYED else pl.ds(j * step, step)
        return held.at[sector, rows, pl.ds(pl.multiple_of(c * Q, 128), Q)]

    def y_copy(d, k, j, source):
        ref = part(near, source, k, j, cm)
        return remote(ref, ref, g_send.at[0], g_recv.at[d - 1, k, j], y_peer(d))

    def y_far(d, k, source):
        ref = part(far, source, k, RELAYED, cm)
        return remote(ref, ref, g_send.at[1], e_recv.at[d - 1, k], y_peer(d))

    def x_copy(d, k, j):
        ref = part(near, d, k, j, cm)
        dst = part(far, d, k, j, cm)
        return remote(ref, dst, g_send.at[2], h_recv.at[d - 1, k, j], x_peer)

    def core_copy(d, k, j, n, c):
        ref = part((near, far)[n], d, k, j, c)
        return remote(ref, ref, g_send.at[3 + n], f_recv.at[n], core_peer)

    for d, k, j in pieces:
        begin(y_copy(d, k, j, 0))
    for d, k in tails:
        begin(y_copy(d, k, RELAYED, 0))
    for d, k in tails:
        begin(y_far(d, k, 0))

    depth_ids = lax.broadcasted_iota(jnp.int32, (1, R), 1)
    chunk = 4 if slots % 4 == 0 else slots

    def first(n_held, zh, g):
        held = (near, far)[n_held]
        for n in range(g * chunk, (g + 1) * chunk):
            t = order[n]
            source = packed[t]
            limit = jnp.where(t < packed[2 * slots], packed[2 * slots + 1 + source], 0)
            keep = jnp.where(depth_ids < limit, 1.0, 0.0).astype(BF16)
            lmat = lbuf[t, zh].reshape(M, R) * keep
            value = jnp.dot(lmat, held[source], preferred_element_type=F32).astype(BF16)
            half[n, zh, :, n_held * H : (n_held + 1) * H] = value

    def second(zh, w):
        for n in range(slots):
            total = lax.dot_general(
                half[n, zh],
                rbuf[order[n], w * H : (w + 1) * H],
                (((1,), (1,)), ((), ())),
                preferred_element_type=F32,
            )
            total = total.reshape(prod.shape[3:])
            if n > 0:
                total = total + prod[zh, w, n - 1] * joins[n]
            prod[zh, w, n] = total

    def core_send(zh, w):
        return remote(
            snd_c.at[zh, w], rcv_c.at[zh, w], r_send.at[0], c_recv.at[zh, w], core_peer
        )

    def spread(zh, w):
        @pl.loop(0, S * K)
        def _(s):
            y, k = s // K, s % K
            away = prod[zh, w, upto[s], co] * has[s]
            snd_c[zh, w, y, k] = away.astype(BF16).reshape(X, Z2, B, H)

        begin(core_send(zh, w))

    handled = []

    def relay_far(count):
        for d, k, j in pieces[len(handled) : len(handled) + count]:
            x_copy(d, k, j).wait_recv()
            begin(core_copy(d, k, j, 1, cm))
            handled.append((d, k, j))

    for n, (d, k, j) in enumerate(pieces):
        y_copy(d, k, j, d).wait_recv()
        begin(x_copy(d, k, j), core_copy(d, k, j, 0, cm))
        if n >= LAG:
            relay_far(1)
    for d, k in tails:
        y_copy(d, k, RELAYED, d).wait_recv()
        begin(core_copy(d, k, RELAYED, 0, cm))
        relay_far(1)
    if Z > 2:
        pl.semaphore_wait(ready.at[0], z_sides)
        if Z > 3:
            signal_sides(ready.at[1])
    relay_far(len(pieces))
    for d, k in tails:
        y_far(d, k, d).wait_recv()
        begin(core_copy(d, k, RELAYED, 1, cm))
    pltpu.make_async_copy(lbuf, lbuf, load_sem.at[3]).wait()
    pltpu.make_async_copy(rbuf, rbuf, load_sem.at[4]).wait()
    others = pl.ds(0, (S - 1) * K)

    def shares(held, rows):
        return held.at[others, rows, pl.ds(0, Q)]

    whole, most, rest = pl.ds(0, R), pl.ds(0, RELAYED * step), pl.ds(0, tail)

    def all_of(held, rows, ssem, rsem, peer):
        return remote(shares(held, rows), shares(held, rows), ssem, rsem, peer)

    def base(zh, w, y, k, x):
        s = y * K + k
        rows = pl.ds(pl.multiple_of(x * Z2 * B, Z2 * B), Z2 * B)
        own = prod[zh, w, upto[s], cm, rows, :] * has[s]
        return own.reshape(Z2, B, H) + rcv_c[zh, w, y, k, x].astype(F32)

    def a1_copy(zh, y):
        at = (zh, y)
        return remote(snd_a1.at[at], rcv_a1.at[at], r_send.at[1], ra1.at[at], x_peer)

    def b1_copy(zh, away, d):
        at = (zh, away, d - 1)
        return remote(snd_b1.at[at], rcv_b1.at[at], r_send.at[2], rb1.at[at], y_peer(d))

    def a2_copy(zh, d, k):
        at = (zh, d - 1, k)
        return remote(snd_a2.at[at], rcv_a2.at[at], r_send.at[3], ra2.at[at], y_peer(d))

    def b2_copy(zh, k):
        at = (zh, k)
        return remote(snd_b2.at[at], rcv_b2.at[at], r_send.at[4], rb2.at[at], x_peer)

    def z_copy(zh, w, k, i):
        z = zh * Z2 + i
        slot = lax.rem(zm - z - 1 + 2 * Z, Z)
        return remote(
            snd_z.at[zh, i, w, k],
            rcv_z.at[w, k, slot],
            z_send.at[zh, i],
            rz.at[w, k],
            dev(z, xm, cm, ym),
        )

    def stage_one_a(zh):
        core_send(zh, 0).wait_recv()
        for d in list(range(1, S)) + [0]:
            y = y_other(d)
            for k in range(K):
                snd_a1[zh, y, k] = base(zh, 0, y, k, xo).astype(BF16)
            begin(a1_copy(zh, y))

    def stage_one_b(zh):
        core_send(zh, 1).wait_recv()
        for away, x in ((0, xo), (1, xm)):
            for d in range(1, S):
                for k in range(K):
                    snd_b1[zh, away, d - 1, k] = base(zh, 1, y_other(d), k, x).astype(BF16)
                begin(b1_copy(zh, away, d))

    def stage_two_a(zh):
        for d in range(1, S):
            yo = y_other(d)
            a1_copy(zh, yo).wait_recv()
            for k in range(K):
                total = base(zh, 0, yo, k, xm) + rcv_a1[zh, yo, k].astype(F32)
                snd_a2[zh, d - 1, k] = total.astype(BF16)
                begin(a2_copy(zh, d, k))

    def stage_two_b(zh):
        for d in range(1, S):
            b1_copy(zh, 0, d).wait_recv()
        for k in range(K):
            total = base(zh, 1, ym, k, xo)
            for d in range(1, S):
                total = total + rcv_b1[zh, 0, d - 1, k].astype(F32)
            snd_b2[zh, k] = total.astype(BF16)
            begin(b2_copy(zh, k))

    def z_own(zh, w, k, i):
        s = ym * K + k
        rows = pl.ds(pl.multiple_of((xm * Z2 + i) * B, B), B)
        total = prod[zh, w, upto[s], cm, rows, :] * has[s]
        total = total + rcv_c[zh, w, ym, k, xm, i].astype(F32)
        if w == 0:
            total = total + rcv_a1[zh, ym, k, i].astype(F32)
            for d in range(1, S):
                total = total + rcv_a2[zh, d - 1, k, i].astype(F32)
        else:
            for d in range(1, S):
                total = total + rcv_b1[zh, 1, d - 1, k, i].astype(F32)
            total = total + rcv_b2[zh, k, i].astype(F32)
        return total

    def stage_three(zh):
        a1_copy(zh, ym).wait_recv()
        for d in range(1, S):
            b1_copy(zh, 1, d).wait_recv()
        for k in range(K):
            for w in range(2):
                if w == 0:
                    for d in range(1, S):
                        a2_copy(zh, d, k).wait_recv()
                else:
                    b2_copy(zh, k).wait_recv()
                for i in range(Z2):
                    @pl.when(zm != zh * Z2 + i)
                    def _():
                        snd_z[zh, i, w, k] = z_own(zh, w, k, i).astype(BF16)
                        begin(z_copy(zh, w, k, i))

    def first_all(n_held, zh):
        for g in range(slots // chunk):
            first(n_held, zh, g)

    all_of(near, whole, g_send.at[3], f_recv.at[0], core_peer).wait_recv()
    first_all(0, 0)
    all_of(far, whole, g_send.at[4], f_recv.at[1], core_peer).wait_recv()
    first_all(1, 0)
    second(0, 0)
    spread(0, 0)
    second(0, 1)
    spread(0, 1)
    stage_one_a(0)
    first_all(0, 1)
    stage_one_b(0)
    first_all(1, 1)
    second(1, 0)
    spread(1, 0)
    second(1, 1)
    spread(1, 1)
    stage_two_a(0)
    stage_two_b(0)
    stage_one_a(1)
    stage_one_b(1)
    for p in range(1, Z - 2):
        pl.semaphore_wait(ready.at[p], z_sides)
        if p + 1 < Z - 2:
            signal_sides(ready.at[p + 1])
    stage_three(0)
    stage_two_a(1)
    stage_two_b(1)
    stage_three(1)

    ids = term * B + lax.broadcasted_iota(jnp.int32, (B, H), 0)
    my_half, my_place = zm // Z2, lax.rem(zm, Z2)
    for k in range(K):
        used = ids < packed[2 * slots + 1 + ym * K + k]
        for w in range(2):
            total = z_own(my_half, w, k, my_place)
            got = rcv_z.at[w, k]
            remote(got, got, r_send.at[0], rz.at[w, k], core_peer).wait_recv()
            for n in range(Z - 1):
                total = total + rcv_z[w, k, n].astype(F32)
            out[k, :, w * H : (w + 1) * H] = jnp.where(used, total, 0.0)

    all_of(near, whole, g_send.at[0], f_recv.at[0], core_peer).wait_send()
    all_of(far, rest, g_send.at[1], f_recv.at[0], core_peer).wait_send()
    all_of(near, most, g_send.at[2], f_recv.at[0], core_peer).wait_send()
    all_of(near, whole, g_send.at[3], f_recv.at[0], core_peer).wait_send()
    all_of(far, whole, g_send.at[4], f_recv.at[0], core_peer).wait_send()
    for n, ref in enumerate((snd_c, snd_a1, snd_b1, snd_a2, snd_b2)):
        remote(ref, ref, r_send.at[n], f_recv.at[0], core_peer).wait_send()
    for zh in range(2):
        for i in range(Z2):
            @pl.when(zm != zh * Z2 + i)
            def _():
                ref = snd_z.at[zh, i]
                remote(ref, ref, z_send.at[zh, i], f_recv.at[0], core_peer).wait_send()


def local(mesh_sizes, wave, left, right, source, target, live, sector_rows):
    T, S = mesh_sizes
    X = 2
    Z = T // (2 * X)
    K, R, C = wave.shape
    B = R // T
    H, Q = C // 2, C // 4
    slots = left.shape[0]
    dims = (Z, X, S, K, B, C)
    left = left.reshape(slots, 2, Z // 2, X, 2, B, R)
    vm = pltpu.VMEM
    dma = pltpu.SemaphoreType.DMA
    Z2 = Z // 2
    share = (K, Z2, B, H)
    scratch = [
        vm((S * K, R, H), BF16),
        vm((S * K, R, H), BF16),
        vm((slots, 2, 2, X, Z2, B, R), BF16),
        vm((slots, C, C), BF16),
        vm((slots, 2, R // 2, C), BF16),
        vm((2, 2, slots, 2, X * Z2 * B, H), F32),
        vm((2, 2, S, K, X, Z2, B, H), BF16),
        vm((2, 2, S, K, X, Z2, B, H), BF16),
        vm((2, S) + share, BF16),
        vm((2, S) + share, BF16),
        vm((2, 2, S - 1) + share, BF16),
        vm((2, 2, S - 1) + share, BF16),
        vm((2, S - 1) + share, BF16),
        vm((2, S - 1) + share, BF16),
        vm((2,) + share, BF16),
        vm((2,) + share, BF16),
        vm((2, Z2, 2, K, B, H), BF16),
        vm((2, K, Z - 1, B, H), BF16),
        pltpu.SMEM((slots,), jnp.int32),
        pltpu.SMEM((slots,), F32),
        pltpu.SMEM((S * K,), jnp.int32),
        pltpu.SMEM((S * K,), F32),
        dma((5,)),
        pltpu.SemaphoreType.REGULAR((max(Z - 2, 1),)),
        dma((5,)),
        dma((S - 1, K, RELAYED + 1)),
        dma((S - 1, K)),
        dma((S - 1, K, RELAYED)),
        dma((2,)),
        dma((5,)),
        dma((2, Z2)),
        dma((2, 2)),
        dma((2, S)),
        dma((2, 2, S - 1)),
        dma((2, S - 1, K)),
        dma((2, K)),
        dma((2, K)),
    ]
    any_spec = pl.BlockSpec(memory_space=pl.ANY)
    smem = pl.BlockSpec(memory_space=pltpu.SMEM)
    return pl.pallas_call(
        functools.partial(kernel, dims),
        out_shape=jax.ShapeDtypeStruct((K, B, C), F32),
        in_specs=[any_spec] * 3 + [smem],
        out_specs=pl.BlockSpec(memory_space=pltpu.VMEM),
        scratch_shapes=scratch,
        compiler_params=pltpu.CompilerParams(
            collective_id=0, has_side_effects=True, vmem_limit_bytes=54784 * 1024
        ),
    )(wave, left, right, jnp.concatenate([source, target, live, sector_rows]))


def solution(mesh):
    in_specs = (
        P("sector", None, None),
        P(("term", "sector"), None, None),
        P(("term", "sector"), None, None),
        P(("term", "sector")),
        P(("term", "sector")),
        P(("term", "sector")),
        P(),
    )
    out_specs = P("sector", "term", None)
    sizes = (mesh.shape["term"], mesh.shape["sector"])
    return jax.shard_map(
        functools.partial(local, sizes),
        mesh=mesh,
        in_specs=in_specs,
        out_specs=out_specs,
        check_vma=False,
    )
```

```python
import functools

import jax
import jax.numpy as jnp
from jax import lax
from jax.experimental import pallas as pl
from jax.experimental.pallas import tpu as pltpu
from jax.sharding import PartitionSpec as P

BF16 = jnp.bfloat16
F32 = jnp.float32
STEPS = 8
RELAYED = 5
LAG = 4


def kernel(
    dims,
    wave,
    left,
    right,
    packed,
    out,
    near,
    far,
    lbuf,
    rbuf,
    half,
    prod,
    snd_c,
    rcv_c,
    snd_a1,
    rcv_a1,
    snd_b1,
    rcv_b1,
    snd_a2,
    rcv_a2,
    snd_b2,
    rcv_b2,
    snd_z,
    rcv_z,
    order,
    joins,
    upto,
    has,
    load_sem,
    ready,
    g_send,
    g_recv,
    e_recv,
    h_recv,
    f_recv,
    r_send,
    z_send,
    c_recv,
    ra1,
    rb1,
    ra2,
    rb2,
    rz,
):
    Z, X, S, K, B, C = dims
    H, Q = C // 2, C // 4
    R = wave.shape[1]
    M = R // 2
    Z2 = Z // 2
    slots = left.shape[0]
    term = lax.axis_index("term")
    ym = lax.axis_index("sector")
    cm = lax.rem(term, 2)
    xm = lax.rem(term // 2, X)
    zm = term // (2 * X)
    co = 1 - cm
    xo = 1 - xm

    def dev(z, x, c, y):
        return ((z * X + x) * 2 + c, y)

    core_peer = dev(zm, xm, co, ym)
    x_peer = dev(zm, xo, cm, ym)

    def y_other(d):
        return lax.rem(ym + d, S)

    def y_peer(d):
        return dev(zm, xm, cm, y_other(d))

    def z_other(d):
        if Z & (Z - 1):
            return lax.rem(zm + d, Z)
        other, bit = zm, 1
        while bit < Z:
            if d & bit:
                other = other + bit * (1 - 2 * lax.rem(zm // bit, 2))
            bit *= 2
        return other

    def z_peer(d):
        return dev(z_other(d), xm, cm, ym)

    def remote(src, dst, ssem, rsem, peer):
        return pltpu.make_async_remote_copy(
            src_ref=src,
            dst_ref=dst,
            send_sem=ssem,
            recv_sem=rsem,
            device_id=peer,
            device_id_type=pl.DeviceIdType.MESH,
        )

    def signal(sem, peer):
        pl.semaphore_signal(sem, inc=1, device_id=peer, device_id_type=pl.DeviceIdType.MESH)

    barrier = pltpu.get_barrier_semaphore()
    z_sides = jnp.where(zm > 0, 1, 0) + jnp.where(zm < Z - 1, 1, 0)

    def signal_sides(sem):
        @pl.when(zm > 0)
        def _():
            signal(sem, dev(zm - 1, xm, cm, ym))

        @pl.when(zm < Z - 1)
        def _():
            signal(sem, dev(zm + 1, xm, cm, ym))

    direct = [core_peer, x_peer] + [y_peer(d) for d in range(1, S)]
    for peer in direct:
        signal(barrier, peer)
    signal_sides(barrier)

    mine = pl.ds(ym * K, K)

    def cols(x):
        return pl.ds(pl.multiple_of(x * H, 128), H)

    own_loads = [
        pltpu.make_async_copy(wave.at[:, :, cols(x)], held.at[mine], load_sem.at[n])
        for n, (x, held) in enumerate(((xm, near), (xo, far)))
    ]
    l_loads = [
        pltpu.make_async_copy(left.at[:, zh, :, x, c], lbuf.at[:, zh, c, x], load_sem.at[3])
        for zh in range(2)
        for x in range(X)
        for c in range(2)
    ]
    r_loads = [
        pltpu.make_async_copy(
            right.at[:, :, cols(x)], rbuf.at[:, :, n * H : (n + 1) * H], load_sem.at[4]
        )
        for n, x in enumerate((xm, xo))
    ]
    for cp in own_loads + l_loads + r_loads:
        cp.start()

    targets = [packed[slots + t] for t in range(slots)]
    ranks = []
    for t in range(slots):
        rank = jnp.int32(0)
        for u in range(slots):
            ahead = targets[u] <= targets[t] if u < t else targets[u] < targets[t]
            if u != t:
                rank = rank + jnp.where(ahead, 1, 0)
        ranks.append(rank)
    before = jnp.int32(-1)
    for n in range(slots):
        slot, target = jnp.int32(0), jnp.int32(0)
        for t in range(slots):
            slot = jnp.where(ranks[t] == n, t, slot)
            target = jnp.where(ranks[t] == n, targets[t], target)
        order[n] = slot
        joins[n] = jnp.where(target == before, 1.0, 0.0)
        before = target
    for s in range(S * K):
        last, below = jnp.int32(0), jnp.int32(0)
        for t in range(slots):
            last = last + jnp.where(targets[t] <= s, 1, 0)
            below = below + jnp.where(targets[t] < s, 1, 0)
        upto[s] = jnp.maximum(last - 1, 0)
        has[s] = jnp.where(last > below, 1.0, 0.0)

    for cp in own_loads:
        cp.wait()
    pl.semaphore_wait(barrier, len(direct) + z_sides)
    if Z > 2:
        signal_sides(ready.at[0])

    step = R // STEPS
    tail = (STEPS - RELAYED) * step
    pieces = [(d, j) for j in range(RELAYED) for d in range(1, S)]
    tails = list(range(1, S))

    def begin(*copies):
        for cp in copies:
            cp.start()

    def part(held, d, j, c):
        sectors = pl.ds(lax.rem(ym + S - d, S) * K, K)
        rows = pl.ds(RELAYED * step, tail) if j == RELAYED else pl.ds(j * step, step)
        return held.at[sectors, rows, pl.ds(pl.multiple_of(c * Q, 128), Q)]

    def y_copy(d, j, source):
        ref = part(near, source, j, cm)
        return remote(ref, ref, g_send.at[0], g_recv.at[d - 1, j], y_peer(d))

    def y_far(d, source):
        ref = part(far, source, RELAYED, cm)
        return remote(ref, ref, g_send.at[1], e_recv.at[d - 1], y_peer(d))

    def x_copy(d, j):
        ref = part(near, d, j, cm)
        dst = part(far, d, j, cm)
        return remote(ref, dst, g_send.at[2], h_recv.at[d - 1, j], x_peer)

    def core_copy(d, j, n, c):
        ref = part((near, far)[n], d, j, c)
        return remote(ref, ref, g_send.at[3 + n], f_recv.at[n], core_peer)

    for d, j in pieces:
        begin(y_copy(d, j, 0))
    for d in tails:
        begin(y_copy(d, RELAYED, 0))
    for d in tails:
        begin(y_far(d, 0))

    depth_ids = lax.broadcasted_iota(jnp.int32, (1, R), 1)
    chunk = 4 if slots % 4 == 0 else slots

    def first(n_held, zh, g):
        held = (near, far)[n_held]
        for n in range(g * chunk, (g + 1) * chunk):
            t = order[n]
            source = packed[t]
            limit = jnp.where(t < packed[2 * slots], packed[2 * slots + 1 + source], 0)
            keep = jnp.where(depth_ids < limit, 1.0, 0.0).astype(BF16)
            lmat = lbuf[t, zh].reshape(M, R) * keep
            value = jnp.dot(lmat, held[source], preferred_element_type=F32).astype(BF16)
            half[n, zh, :, n_held * H : (n_held + 1) * H] = value

    def second(zh, w):
        for n in range(slots):
            total = lax.dot_general(
                half[n, zh],
                rbuf[order[n], w * H : (w + 1) * H],
                (((1,), (1,)), ((), ())),
                preferred_element_type=F32,
            )
            total = total.reshape(prod.shape[3:])
            if n > 0:
                total = total + prod[zh, w, n - 1] * joins[n]
            prod[zh, w, n] = total

    def core_send(zh, w):
        return remote(
            snd_c.at[zh, w], rcv_c.at[zh, w], r_send.at[0], c_recv.at[zh, w], core_peer
        )

    def spread(zh, w):
        @pl.loop(0, S * K)
        def _(s):
            y, k = s // K, s % K
            away = prod[zh, w, upto[s], co] * has[s]
            snd_c[zh, w, y, k] = away.astype(BF16).reshape(X, Z2, B, H)

        begin(core_send(zh, w))

    handled = []

    def relay_far(count):
        for d, j in pieces[len(handled) : len(handled) + count]:
            x_copy(d, j).wait_recv()
            begin(core_copy(d, j, 1, cm))
            handled.append((d, j))

    for n, (d, j) in enumerate(pieces):
        y_copy(d, j, d).wait_recv()
        begin(x_copy(d, j), core_copy(d, j, 0, cm))
        if n >= LAG:
            relay_far(1)
    for d in tails:
        y_copy(d, RELAYED, d).wait_recv()
        begin(core_copy(d, RELAYED, 0, cm))
        relay_far(1)
    if Z > 2:
        pl.semaphore_wait(ready.at[0], z_sides)
        if Z > 3:
            signal_sides(ready.at[1])
    relay_far(len(pieces))
    for d in tails:
        y_far(d, d).wait_recv()
        begin(core_copy(d, RELAYED, 1, cm))
    pltpu.make_async_copy(lbuf, lbuf, load_sem.at[3]).wait()
    pltpu.make_async_copy(rbuf, rbuf, load_sem.at[4]).wait()
    others = pl.ds(0, (S - 1) * K)

    def shares(held, rows):
        return held.at[others, rows, pl.ds(0, Q)]

    whole, most, rest = pl.ds(0, R), pl.ds(0, RELAYED * step), pl.ds(0, tail)

    def all_of(held, rows, ssem, rsem, peer):
        return remote(shares(held, rows), shares(held, rows), ssem, rsem, peer)

    def base(zh, w, y, k, x):
        s = y * K + k
        rows = pl.ds(pl.multiple_of(x * Z2 * B, Z2 * B), Z2 * B)
        own = prod[zh, w, upto[s], cm, rows, :] * has[s]
        return own.reshape(Z2, B, H) + rcv_c[zh, w, y, k, x].astype(F32)

    def a1_copy(zh, y):
        at = (zh, y)
        return remote(snd_a1.at[at], rcv_a1.at[at], r_send.at[1], ra1.at[at], x_peer)

    def b1_copy(zh, away, d):
        at = (zh, away, d - 1)
        return remote(snd_b1.at[at], rcv_b1.at[at], r_send.at[2], rb1.at[at], y_peer(d))

    def a2_copy(zh, d, k):
        at = (zh, d - 1, k)
        return remote(snd_a2.at[at], rcv_a2.at[at], r_send.at[3], ra2.at[at], y_peer(d))

    def b2_copy(zh, k):
        at = (zh, k)
        return remote(snd_b2.at[at], rcv_b2.at[at], r_send.at[4], rb2.at[at], x_peer)

    def z_copy(zh, w, k, i):
        z = zh * Z2 + i
        slot = lax.rem(zm - z - 1 + 2 * Z, Z)
        return remote(
            snd_z.at[zh, i, w, k],
            rcv_z.at[w, k, slot],
            z_send.at[zh, i],
            rz.at[w, k],
            dev(z, xm, cm, ym),
        )

    def stage_one_a(zh):
        core_send(zh, 0).wait_recv()
        for d in list(range(1, S)) + [0]:
            y = y_other(d)
            for k in range(K):
                snd_a1[zh, y, k] = base(zh, 0, y, k, xo).astype(BF16)
            begin(a1_copy(zh, y))

    def stage_one_b(zh):
        core_send(zh, 1).wait_recv()
        for away, x in ((0, xo), (1, xm)):
            for d in range(1, S):
                for k in range(K):
                    snd_b1[zh, away, d - 1, k] = base(zh, 1, y_other(d), k, x).astype(BF16)
                begin(b1_copy(zh, away, d))

    def stage_two_a(zh):
        for d in range(1, S):
            yo = y_other(d)
            a1_copy(zh, yo).wait_recv()
            for k in range(K):
                total = base(zh, 0, yo, k, xm) + rcv_a1[zh, yo, k].astype(F32)
                snd_a2[zh, d - 1, k] = total.astype(BF16)
                begin(a2_copy(zh, d, k))

    def stage_two_b(zh):
        for d in range(1, S):
            b1_copy(zh, 0, d).wait_recv()
        for k in range(K):
            total = base(zh, 1, ym, k, xo)
            for d in range(1, S):
                total = total + rcv_b1[zh, 0, d - 1, k].astype(F32)
            snd_b2[zh, k] = total.astype(BF16)
            begin(b2_copy(zh, k))

    def z_own(zh, w, k, i):
        s = ym * K + k
        rows = pl.ds(pl.multiple_of((xm * Z2 + i) * B, B), B)
        total = prod[zh, w, upto[s], cm, rows, :] * has[s]
        total = total + rcv_c[zh, w, ym, k, xm, i].astype(F32)
        if w == 0:
            total = total + rcv_a1[zh, ym, k, i].astype(F32)
            for d in range(1, S):
                total = total + rcv_a2[zh, d - 1, k, i].astype(F32)
        else:
            for d in range(1, S):
                total = total + rcv_b1[zh, 1, d - 1, k, i].astype(F32)
            total = total + rcv_b2[zh, k, i].astype(F32)
        return total

    def stage_three(zh):
        a1_copy(zh, ym).wait_recv()
        for d in range(1, S):
            b1_copy(zh, 1, d).wait_recv()
        for k in range(K):
            for w in range(2):
                if w == 0:
                    for d in range(1, S):
                        a2_copy(zh, d, k).wait_recv()
                else:
                    b2_copy(zh, k).wait_recv()
                for i in range(Z2):
                    @pl.when(zm != zh * Z2 + i)
                    def _():
                        snd_z[zh, i, w, k] = z_own(zh, w, k, i).astype(BF16)
                        begin(z_copy(zh, w, k, i))

    def first_all(n_held, zh):
        for g in range(slots // chunk):
            first(n_held, zh, g)

    all_of(near, whole, g_send.at[3], f_recv.at[0], core_peer).wait_recv()
    first_all(0, 0)
    all_of(far, whole, g_send.at[4], f_recv.at[1], core_peer).wait_recv()
    first_all(1, 0)
    second(0, 0)
    spread(0, 0)
    second(0, 1)
    spread(0, 1)
    stage_one_a(0)
    first_all(0, 1)
    stage_one_b(0)
    first_all(1, 1)
    second(1, 0)
    spread(1, 0)
    second(1, 1)
    spread(1, 1)
    stage_two_a(0)
    stage_two_b(0)
    stage_one_a(1)
    stage_one_b(1)
    for p in range(1, Z - 2):
        pl.semaphore_wait(ready.at[p], z_sides)
        if p + 1 < Z - 2:
            signal_sides(ready.at[p + 1])
    stage_three(0)
    stage_two_a(1)
    stage_two_b(1)
    stage_three(1)

    ids = term * B + lax.broadcasted_iota(jnp.int32, (B, H), 0)
    my_half, my_place = zm // Z2, lax.rem(zm, Z2)
    for k in range(K):
        used = ids < packed[2 * slots + 1 + ym * K + k]
        for w in range(2):
            total = z_own(my_half, w, k, my_place)
            got = rcv_z.at[w, k]
            remote(got, got, r_send.at[0], rz.at[w, k], core_peer).wait_recv()
            for n in range(Z - 1):
                total = total + rcv_z[w, k, n].astype(F32)
            out[k, :, w * H : (w + 1) * H] = jnp.where(used, total, 0.0)

    all_of(near, whole, g_send.at[0], f_recv.at[0], core_peer).wait_send()
    all_of(far, rest, g_send.at[1], f_recv.at[0], core_peer).wait_send()
    all_of(near, most, g_send.at[2], f_recv.at[0], core_peer).wait_send()
    all_of(near, whole, g_send.at[3], f_recv.at[0], core_peer).wait_send()
    all_of(far, whole, g_send.at[4], f_recv.at[0], core_peer).wait_send()
    for n, ref in enumerate((snd_c, snd_a1, snd_b1, snd_a2, snd_b2)):
        remote(ref, ref, r_send.at[n], f_recv.at[0], core_peer).wait_send()
    for zh in range(2):
        for i in range(Z2):
            @pl.when(zm != zh * Z2 + i)
            def _():
                ref = snd_z.at[zh, i]
                remote(ref, ref, z_send.at[zh, i], f_recv.at[0], core_peer).wait_send()


def local(mesh_sizes, wave, left, right, source, target, live, sector_rows):
    T, S = mesh_sizes
    X = 2
    Z = T // (2 * X)
    K, R, C = wave.shape
    B = R // T
    H, Q = C // 2, C // 4
    slots = left.shape[0]
    dims = (Z, X, S, K, B, C)
    left = left.reshape(slots, 2, Z // 2, X, 2, B, R)
    vm = pltpu.VMEM
    dma = pltpu.SemaphoreType.DMA
    Z2 = Z // 2
    share = (K, Z2, B, H)
    scratch = [
        vm((S * K, R, H), BF16),
        vm((S * K, R, H), BF16),
        vm((slots, 2, 2, X, Z2, B, R), BF16),
        vm((slots, C, C), BF16),
        vm((slots, 2, R // 2, C), BF16),
        vm((2, 2, slots, 2, X * Z2 * B, H), F32),
        vm((2, 2, S, K, X, Z2, B, H), BF16),
        vm((2, 2, S, K, X, Z2, B, H), BF16),
        vm((2, S) + share, BF16),
        vm((2, S) + share, BF16),
        vm((2, 2, S - 1) + share, BF16),
        vm((2, 2, S - 1) + share, BF16),
        vm((2, S - 1) + share, BF16),
        vm((2, S - 1) + share, BF16),
        vm((2,) + share, BF16),
        vm((2,) + share, BF16),
        vm((2, Z2, 2, K, B, H), BF16),
        vm((2, K, Z - 1, B, H), BF16),
        pltpu.SMEM((slots,), jnp.int32),
        pltpu.SMEM((slots,), F32),
        pltpu.SMEM((S * K,), jnp.int32),
        pltpu.SMEM((S * K,), F32),
        dma((5,)),
        pltpu.SemaphoreType.REGULAR((max(Z - 2, 1),)),
        dma((5,)),
        dma((S - 1, RELAYED + 1)),
        dma((S - 1,)),
        dma((S - 1, RELAYED)),
        dma((2,)),
        dma((5,)),
        dma((2, Z2)),
        dma((2, 2)),
        dma((2, S)),
        dma((2, 2, S - 1)),
        dma((2, S - 1, K)),
        dma((2, K)),
        dma((2, K)),
    ]
    any_spec = pl.BlockSpec(memory_space=pl.ANY)
    smem = pl.BlockSpec(memory_space=pltpu.SMEM)
    return pl.pallas_call(
        functools.partial(kernel, dims),
        out_shape=jax.ShapeDtypeStruct((K, B, C), F32),
        in_specs=[any_spec] * 3 + [smem],
        out_specs=pl.BlockSpec(memory_space=pltpu.VMEM),
        scratch_shapes=scratch,
        compiler_params=pltpu.CompilerParams(
            collective_id=0, has_side_effects=True, vmem_limit_bytes=54784 * 1024
        ),
    )(wave, left, right, jnp.concatenate([source, target, live, sector_rows]))


def solution(mesh):
    in_specs = (
        P("sector", None, None),
        P(("term", "sector"), None, None),
        P(("term", "sector"), None, None),
        P(("term", "sector")),
        P(("term", "sector")),
        P(("term", "sector")),
        P(),
    )
    out_specs = P("sector", "term", None)
    sizes = (mesh.shape["term"], mesh.shape["sector"])
    return jax.shard_map(
        functools.partial(local, sizes),
        mesh=mesh,
        in_specs=in_specs,
        out_specs=out_specs,
        check_vma=False,
    )
```

```python
import functools

import jax
import jax.numpy as jnp
from jax import lax
from jax.experimental import pallas as pl
from jax.experimental.pallas import tpu as pltpu
from jax.sharding import PartitionSpec as P

BF16 = jnp.bfloat16
F32 = jnp.float32
STEPS = 16
RELAYED = 11
LAG = 9


def kernel(
    dims,
    wave,
    left,
    right,
    packed,
    out,
    near,
    far,
    lbuf,
    rbuf,
    half,
    prod,
    snd_c,
    rcv_c,
    snd_a1,
    rcv_a1,
    snd_b1,
    rcv_b1,
    snd_a2,
    rcv_a2,
    snd_b2,
    rcv_b2,
    snd_z,
    rcv_z,
    order,
    joins,
    upto,
    has,
    load_sem,
    ready,
    g_send,
    g_recv,
    e_recv,
    h_recv,
    f_recv,
    r_send,
    z_send,
    c_recv,
    ra1,
    rb1,
    ra2,
    rb2,
    rz,
):
    Z, X, S, K, B, C = dims
    H, Q = C // 2, C // 4
    R = wave.shape[1]
    M = R // 2
    Z2 = Z // 2
    slots = left.shape[0]
    term = lax.axis_index("term")
    ym = lax.axis_index("sector")
    cm = lax.rem(term, 2)
    xm = lax.rem(term // 2, X)
    zm = term // (2 * X)
    co = 1 - cm
    xo = 1 - xm

    def dev(z, x, c, y):
        return ((z * X + x) * 2 + c, y)

    core_peer = dev(zm, xm, co, ym)
    x_peer = dev(zm, xo, cm, ym)

    def y_other(d):
        return lax.rem(ym + d, S)

    def y_peer(d):
        return dev(zm, xm, cm, y_other(d))

    def z_other(d):
        if Z & (Z - 1):
            return lax.rem(zm + d, Z)
        other, bit = zm, 1
        while bit < Z:
            if d & bit:
                other = other + bit * (1 - 2 * lax.rem(zm // bit, 2))
            bit *= 2
        return other

    def z_peer(d):
        return dev(z_other(d), xm, cm, ym)

    def remote(src, dst, ssem, rsem, peer):
        return pltpu.make_async_remote_copy(
            src_ref=src,
            dst_ref=dst,
            send_sem=ssem,
            recv_sem=rsem,
            device_id=peer,
            device_id_type=pl.DeviceIdType.MESH,
        )

    def signal(sem, peer):
        pl.semaphore_signal(sem, inc=1, device_id=peer, device_id_type=pl.DeviceIdType.MESH)

    barrier = pltpu.get_barrier_semaphore()
    z_sides = jnp.where(zm > 0, 1, 0) + jnp.where(zm < Z - 1, 1, 0)

    def signal_sides(sem):
        @pl.when(zm > 0)
        def _():
            signal(sem, dev(zm - 1, xm, cm, ym))

        @pl.when(zm < Z - 1)
        def _():
            signal(sem, dev(zm + 1, xm, cm, ym))

    direct = [core_peer, x_peer] + [y_peer(d) for d in range(1, S)]
    for peer in direct:
        signal(barrier, peer)
    signal_sides(barrier)

    mine = pl.ds(ym * K, K)

    def cols(x):
        return pl.ds(pl.multiple_of(x * H, 128), H)

    own_loads = [
        pltpu.make_async_copy(wave.at[:, :, cols(x)], held.at[mine], load_sem.at[n])
        for n, (x, held) in enumerate(((xm, near), (xo, far)))
    ]
    l_loads = [
        pltpu.make_async_copy(left.at[:, zh, :, x, c], lbuf.at[:, zh, c, x], load_sem.at[3])
        for zh in range(2)
        for x in range(X)
        for c in range(2)
    ]
    r_loads = [
        pltpu.make_async_copy(
            right.at[:, :, cols(x)], rbuf.at[:, :, n * H : (n + 1) * H], load_sem.at[4]
        )
        for n, x in enumerate((xm, xo))
    ]
    for cp in own_loads + l_loads + r_loads:
        cp.start()

    targets = [packed[slots + t] for t in range(slots)]
    ranks = []
    for t in range(slots):
        rank = jnp.int32(0)
        for u in range(slots):
            ahead = targets[u] <= targets[t] if u < t else targets[u] < targets[t]
            if u != t:
                rank = rank + jnp.where(ahead, 1, 0)
        ranks.append(rank)
    before = jnp.int32(-1)
    for n in range(slots):
        slot, target = jnp.int32(0), jnp.int32(0)
        for t in range(slots):
            slot = jnp.where(ranks[t] == n, t, slot)
            target = jnp.where(ranks[t] == n, targets[t], target)
        order[n] = slot
        joins[n] = jnp.where(target == before, 1.0, 0.0)
        before = target
    for s in range(S * K):
        last, below = jnp.int32(0), jnp.int32(0)
        for t in range(slots):
            last = last + jnp.where(targets[t] <= s, 1, 0)
            below = below + jnp.where(targets[t] < s, 1, 0)
        upto[s] = jnp.maximum(last - 1, 0)
        has[s] = jnp.where(last > below, 1.0, 0.0)

    for cp in own_loads:
        cp.wait()
    pl.semaphore_wait(barrier, len(direct) + z_sides)
    if Z > 2:
        signal_sides(ready.at[0])

    step = R // STEPS
    tail = (STEPS - RELAYED) * step
    pieces = [(d, j) for j in range(RELAYED) for d in range(1, S)]
    tails = list(range(1, S))

    def begin(*copies):
        for cp in copies:
            cp.start()

    def part(held, d, j, c):
        sectors = pl.ds(lax.rem(ym + S - d, S) * K, K)
        rows = pl.ds(RELAYED * step, tail) if j == RELAYED else pl.ds(j * step, step)
        return held.at[sectors, rows, pl.ds(pl.multiple_of(c * Q, 128), Q)]

    def y_copy(d, j, source):
        ref = part(near, source, j, cm)
        return remote(ref, ref, g_send.at[0], g_recv.at[d - 1, j], y_peer(d))

    def y_far(d, source):
        ref = part(far, source, RELAYED, cm)
        return remote(ref, ref, g_send.at[1], e_recv.at[d - 1], y_peer(d))

    def x_copy(d, j):
        ref = part(near, d, j, cm)
        dst = part(far, d, j, cm)
        return remote(ref, dst, g_send.at[2], h_recv.at[d - 1, j], x_peer)

    def core_copy(d, j, n, c):
        ref = part((near, far)[n], d, j, c)
        return remote(ref, ref, g_send.at[3 + n], f_recv.at[n], core_peer)

    for d, j in pieces:
        begin(y_copy(d, j, 0))
    for d in tails:
        begin(y_copy(d, RELAYED, 0))
    for d in tails:
        begin(y_far(d, 0))

    depth_ids = lax.broadcasted_iota(jnp.int32, (1, R), 1)
    chunk = 4 if slots % 4 == 0 else slots

    def first(n_held, zh, g):
        held = (near, far)[n_held]
        for n in range(g * chunk, (g + 1) * chunk):
            t = order[n]
            source = packed[t]
            limit = jnp.where(t < packed[2 * slots], packed[2 * slots + 1 + source], 0)
            keep = jnp.where(depth_ids < limit, 1.0, 0.0).astype(BF16)
            lmat = lbuf[t, zh].reshape(M, R) * keep
            value = jnp.dot(lmat, held[source], preferred_element_type=F32).astype(BF16)
            half[n, zh, :, n_held * H : (n_held + 1) * H] = value

    def second(zh, w):
        for n in range(slots):
            total = lax.dot_general(
                half[n, zh],
                rbuf[order[n], w * H : (w + 1) * H],
                (((1,), (1,)), ((), ())),
                preferred_element_type=F32,
            )
            total = total.reshape(prod.shape[3:])
            if n > 0:
                total = total + prod[zh, w, n - 1] * joins[n]
            prod[zh, w, n] = total

    def core_send(zh, w):
        return remote(
            snd_c.at[zh, w], rcv_c.at[zh, w], r_send.at[0], c_recv.at[zh, w], core_peer
        )

    def spread(zh, w):
        @pl.loop(0, S * K, unroll=4)
        def _(s):
            y, k = s // K, s % K
            away = prod[zh, w, upto[s], co] * has[s]
            snd_c[zh, w, y, k] = away.astype(BF16).reshape(X, Z2, B, H)

        begin(core_send(zh, w))

    handled = []

    def relay_far(count):
        for d, j in pieces[len(handled) : len(handled) + count]:
            x_copy(d, j).wait_recv()
            begin(core_copy(d, j, 1, cm))
            handled.append((d, j))

    for n, (d, j) in enumerate(pieces):
        y_copy(d, j, d).wait_recv()
        begin(x_copy(d, j), core_copy(d, j, 0, cm))
        if n >= LAG:
            relay_far(1)
    for d in tails:
        y_copy(d, RELAYED, d).wait_recv()
        begin(core_copy(d, RELAYED, 0, cm))
        relay_far(1)
    if Z > 2:
        pl.semaphore_wait(ready.at[0], z_sides)
        if Z > 3:
            signal_sides(ready.at[1])
    relay_far(len(pieces))
    for d in tails:
        y_far(d, d).wait_recv()
        begin(core_copy(d, RELAYED, 1, cm))
    pltpu.make_async_copy(lbuf, lbuf, load_sem.at[3]).wait()
    pltpu.make_async_copy(rbuf, rbuf, load_sem.at[4]).wait()
    others = pl.ds(0, (S - 1) * K)

    def shares(held, rows):
        return held.at[others, rows, pl.ds(0, Q)]

    whole, most, rest = pl.ds(0, R), pl.ds(0, RELAYED * step), pl.ds(0, tail)

    def all_of(held, rows, ssem, rsem, peer):
        return remote(shares(held, rows), shares(held, rows), ssem, rsem, peer)

    def base(zh, w, y, k, x):
        s = y * K + k
        rows = pl.ds(pl.multiple_of(x * Z2 * B, Z2 * B), Z2 * B)
        own = prod[zh, w, upto[s], cm, rows, :] * has[s]
        return own.reshape(Z2, B, H) + rcv_c[zh, w, y, k, x].astype(F32)

    def a1_copy(zh, y):
        at = (zh, y)
        return remote(snd_a1.at[at], rcv_a1.at[at], r_send.at[1], ra1.at[at], x_peer)

    def b1_copy(zh, away, d):
        at = (zh, away, d - 1)
        return remote(snd_b1.at[at], rcv_b1.at[at], r_send.at[2], rb1.at[at], y_peer(d))

    def a2_copy(zh, d, k):
        at = (zh, d - 1, k)
        return remote(snd_a2.at[at], rcv_a2.at[at], r_send.at[3], ra2.at[at], y_peer(d))

    def b2_copy(zh, k):
        at = (zh, k)
        return remote(snd_b2.at[at], rcv_b2.at[at], r_send.at[4], rb2.at[at], x_peer)

    def z_copy(zh, w, k, i):
        z = zh * Z2 + i
        slot = lax.rem(zm - z - 1 + 2 * Z, Z)
        return remote(
            snd_z.at[zh, i, w, k],
            rcv_z.at[w, k, slot],
            z_send.at[zh, i],
            rz.at[w, k],
            dev(z, xm, cm, ym),
        )

    def stage_one_a(zh):
        core_send(zh, 0).wait_recv()
        for d in list(range(1, S)) + [0]:
            y = y_other(d)
            for k in range(K):
                snd_a1[zh, y, k] = base(zh, 0, y, k, xo).astype(BF16)
            begin(a1_copy(zh, y))

    def stage_one_b(zh):
        core_send(zh, 1).wait_recv()
        for away, x in ((0, xo), (1, xm)):
            for d in range(1, S):
                for k in range(K):
                    snd_b1[zh, away, d - 1, k] = base(zh, 1, y_other(d), k, x).astype(BF16)
                begin(b1_copy(zh, away, d))

    def stage_two_a(zh):
        for d in range(1, S):
            yo = y_other(d)
            a1_copy(zh, yo).wait_recv()
            for k in range(K):
                total = base(zh, 0, yo, k, xm) + rcv_a1[zh, yo, k].astype(F32)
                snd_a2[zh, d - 1, k] = total.astype(BF16)
                begin(a2_copy(zh, d, k))

    def stage_two_b(zh):
        for d in range(1, S):
            b1_copy(zh, 0, d).wait_recv()
        for k in range(K):
            total = base(zh, 1, ym, k, xo)
            for d in range(1, S):
                total = total + rcv_b1[zh, 0, d - 1, k].astype(F32)
            snd_b2[zh, k] = total.astype(BF16)
            begin(b2_copy(zh, k))

    def z_own(zh, w, k, i):
        s = ym * K + k
        rows = pl.ds(pl.multiple_of((xm * Z2 + i) * B, B), B)
        total = prod[zh, w, upto[s], cm, rows, :] * has[s]
        total = total + rcv_c[zh, w, ym, k, xm, i].astype(F32)
        if w == 0:
            total = total + rcv_a1[zh, ym, k, i].astype(F32)
            for d in range(1, S):
                total = total + rcv_a2[zh, d - 1, k, i].astype(F32)
        else:
            for d in range(1, S):
                total = total + rcv_b1[zh, 1, d - 1, k, i].astype(F32)
            total = total + rcv_b2[zh, k, i].astype(F32)
        return total

    def stage_three(zh):
        a1_copy(zh, ym).wait_recv()
        for d in range(1, S):
            b1_copy(zh, 1, d).wait_recv()
        for k in range(K):
            for w in range(2):
                if w == 0:
                    for d in range(1, S):
                        a2_copy(zh, d, k).wait_recv()
                else:
                    b2_copy(zh, k).wait_recv()
                for i in range(Z2):
                    @pl.when(zm != zh * Z2 + i)
                    def _():
                        snd_z[zh, i, w, k] = z_own(zh, w, k, i).astype(BF16)
                        begin(z_copy(zh, w, k, i))

    def first_all(n_held, zh):
        for g in range(slots // chunk):
            first(n_held, zh, g)

    all_of(near, whole, g_send.at[3], f_recv.at[0], core_peer).wait_recv()
    first_all(0, 0)
    all_of(far, whole, g_send.at[4], f_recv.at[1], core_peer).wait_recv()
    first_all(1, 0)
    second(0, 0)
    spread(0, 0)
    second(0, 1)
    spread(0, 1)
    stage_one_a(0)
    first_all(0, 1)
    stage_one_b(0)
    first_all(1, 1)
    second(1, 0)
    spread(1, 0)
    second(1, 1)
    spread(1, 1)
    stage_two_a(0)
    stage_two_b(0)
    stage_one_a(1)
    stage_one_b(1)
    for p in range(1, Z - 2):
        pl.semaphore_wait(ready.at[p], z_sides)
        if p + 1 < Z - 2:
            signal_sides(ready.at[p + 1])
    stage_three(0)
    stage_two_a(1)
    stage_two_b(1)
    stage_three(1)

    ids = term * B + lax.broadcasted_iota(jnp.int32, (B, H), 0)
    my_half, my_place = zm // Z2, lax.rem(zm, Z2)
    for k in range(K):
        used = ids < packed[2 * slots + 1 + ym * K + k]
        for w in range(2):
            total = z_own(my_half, w, k, my_place)
            got = rcv_z.at[w, k]
            remote(got, got, r_send.at[0], rz.at[w, k], core_peer).wait_recv()
            for n in range(Z - 1):
                total = total + rcv_z[w, k, n].astype(F32)
            out[k, :, w * H : (w + 1) * H] = jnp.where(used, total, 0.0)

    all_of(near, whole, g_send.at[0], f_recv.at[0], core_peer).wait_send()
    all_of(far, rest, g_send.at[1], f_recv.at[0], core_peer).wait_send()
    all_of(near, most, g_send.at[2], f_recv.at[0], core_peer).wait_send()
    all_of(near, whole, g_send.at[3], f_recv.at[0], core_peer).wait_send()
    all_of(far, whole, g_send.at[4], f_recv.at[0], core_peer).wait_send()
    for n, ref in enumerate((snd_c, snd_a1, snd_b1, snd_a2, snd_b2)):
        remote(ref, ref, r_send.at[n], f_recv.at[0], core_peer).wait_send()
    for zh in range(2):
        for i in range(Z2):
            @pl.when(zm != zh * Z2 + i)
            def _():
                ref = snd_z.at[zh, i]
                remote(ref, ref, z_send.at[zh, i], f_recv.at[0], core_peer).wait_send()


def local(mesh_sizes, wave, left, right, source, target, live, sector_rows):
    T, S = mesh_sizes
    X = 2
    Z = T // (2 * X)
    K, R, C = wave.shape
    B = R // T
    H, Q = C // 2, C // 4
    slots = left.shape[0]
    dims = (Z, X, S, K, B, C)
    left = left.reshape(slots, 2, Z // 2, X, 2, B, R)
    vm = pltpu.VMEM
    dma = pltpu.SemaphoreType.DMA
    Z2 = Z // 2
    share = (K, Z2, B, H)
    scratch = [
        vm((S * K, R, H), BF16),
        vm((S * K, R, H), BF16),
        vm((slots, 2, 2, X, Z2, B, R), BF16),
        vm((slots, C, C), BF16),
        vm((slots, 2, R // 2, C), BF16),
        vm((2, 2, slots, 2, X * Z2 * B, H), F32),
        vm((2, 2, S, K, X, Z2, B, H), BF16),
        vm((2, 2, S, K, X, Z2, B, H), BF16),
        vm((2, S) + share, BF16),
        vm((2, S) + share, BF16),
        vm((2, 2, S - 1) + share, BF16),
        vm((2, 2, S - 1) + share, BF16),
        vm((2, S - 1) + share, BF16),
        vm((2, S - 1) + share, BF16),
        vm((2,) + share, BF16),
        vm((2,) + share, BF16),
        vm((2, Z2, 2, K, B, H), BF16),
        vm((2, K, Z - 1, B, H), BF16),
        pltpu.SMEM((slots,), jnp.int32),
        pltpu.SMEM((slots,), F32),
        pltpu.SMEM((S * K,), jnp.int32),
        pltpu.SMEM((S * K,), F32),
        dma((5,)),
        pltpu.SemaphoreType.REGULAR((max(Z - 2, 1),)),
        dma((5,)),
        dma((S - 1, RELAYED + 1)),
        dma((S - 1,)),
        dma((S - 1, RELAYED)),
        dma((2,)),
        dma((5,)),
        dma((2, Z2)),
        dma((2, 2)),
        dma((2, S)),
        dma((2, 2, S - 1)),
        dma((2, S - 1, K)),
        dma((2, K)),
        dma((2, K)),
    ]
    any_spec = pl.BlockSpec(memory_space=pl.ANY)
    smem = pl.BlockSpec(memory_space=pltpu.SMEM)
    return pl.pallas_call(
        functools.partial(kernel, dims),
        out_shape=jax.ShapeDtypeStruct((K, B, C), F32),
        in_specs=[any_spec] * 3 + [smem],
        out_specs=pl.BlockSpec(memory_space=pltpu.VMEM),
        scratch_shapes=scratch,
        compiler_params=pltpu.CompilerParams(
            collective_id=0, has_side_effects=True, vmem_limit_bytes=54784 * 1024
        ),
    )(wave, left, right, jnp.concatenate([source, target, live, sector_rows]))


def solution(mesh):
    in_specs = (
        P("sector", None, None),
        P(("term", "sector"), None, None),
        P(("term", "sector"), None, None),
        P(("term", "sector")),
        P(("term", "sector")),
        P(("term", "sector")),
        P(),
    )
    out_specs = P("sector", "term", None)
    sizes = (mesh.shape["term"], mesh.shape["sector"])
    return jax.shard_map(
        functools.partial(local, sizes),
        mesh=mesh,
        in_specs=in_specs,
        out_specs=out_specs,
        check_vma=False,
    )
```

```python
import functools

import jax
import jax.numpy as jnp
from jax import lax
from jax.experimental import pallas as pl
from jax.experimental.pallas import tpu as pltpu
from jax.sharding import PartitionSpec as P

BF16 = jnp.bfloat16
F32 = jnp.float32
STEPS = 16
RELAYED = 11
LAG = 11


def kernel(
    dims,
    wave,
    left,
    right,
    packed,
    out,
    near,
    far,
    lbuf,
    rbuf,
    half,
    prod,
    snd_c,
    rcv_c,
    snd_a1,
    rcv_a1,
    snd_b1,
    rcv_b1,
    snd_a2,
    rcv_a2,
    snd_b2,
    rcv_b2,
    snd_z,
    rcv_z,
    order,
    joins,
    upto,
    has,
    load_sem,
    ready,
    g_send,
    g_recv,
    e_recv,
    h_recv,
    f_recv,
    r_send,
    z_send,
    c_recv,
    ra1,
    rb1,
    ra2,
    rb2,
    rz,
):
    Z, X, S, K, B, C = dims
    H, Q = C // 2, C // 4
    R = wave.shape[1]
    M = R // 2
    Z2 = Z // 2
    slots = left.shape[0]
    term = lax.axis_index("term")
    ym = lax.axis_index("sector")
    cm = lax.rem(term, 2)
    xm = lax.rem(term // 2, X)
    zm = term // (2 * X)
    co = 1 - cm
    xo = 1 - xm

    def dev(z, x, c, y):
        return ((z * X + x) * 2 + c, y)

    core_peer = dev(zm, xm, co, ym)
    x_peer = dev(zm, xo, cm, ym)

    def y_other(d):
        return lax.rem(ym + d, S)

    def y_peer(d):
        return dev(zm, xm, cm, y_other(d))

    def z_other(d):
        if Z & (Z - 1):
            return lax.rem(zm + d, Z)
        other, bit = zm, 1
        while bit < Z:
            if d & bit:
                other = other + bit * (1 - 2 * lax.rem(zm // bit, 2))
            bit *= 2
        return other

    def z_peer(d):
        return dev(z_other(d), xm, cm, ym)

    def remote(src, dst, ssem, rsem, peer):
        return pltpu.make_async_remote_copy(
            src_ref=src,
            dst_ref=dst,
            send_sem=ssem,
            recv_sem=rsem,
            device_id=peer,
            device_id_type=pl.DeviceIdType.MESH,
        )

    def signal(sem, peer):
        pl.semaphore_signal(sem, inc=1, device_id=peer, device_id_type=pl.DeviceIdType.MESH)

    barrier = pltpu.get_barrier_semaphore()
    z_sides = jnp.where(zm > 0, 1, 0) + jnp.where(zm < Z - 1, 1, 0)

    def signal_sides(sem):
        @pl.when(zm > 0)
        def _():
            signal(sem, dev(zm - 1, xm, cm, ym))

        @pl.when(zm < Z - 1)
        def _():
            signal(sem, dev(zm + 1, xm, cm, ym))

    direct = [core_peer, x_peer] + [y_peer(d) for d in range(1, S)]
    for peer in direct:
        signal(barrier, peer)
    signal_sides(barrier)

    mine = pl.ds(ym * K, K)

    def cols(x):
        return pl.ds(pl.multiple_of(x * H, 128), H)

    own_loads = [
        pltpu.make_async_copy(wave.at[:, :, cols(x)], held.at[mine], load_sem.at[n])
        for n, (x, held) in enumerate(((xm, near), (xo, far)))
    ]
    l_loads = [
        pltpu.make_async_copy(left.at[:, zh, :, x, c], lbuf.at[:, zh, c, x], load_sem.at[3])
        for zh in range(2)
        for x in range(X)
        for c in range(2)
    ]
    r_loads = [
        pltpu.make_async_copy(
            right.at[:, :, cols(x)], rbuf.at[:, :, n * H : (n + 1) * H], load_sem.at[4]
        )
        for n, x in enumerate((xm, xo))
    ]
    for cp in own_loads + l_loads + r_loads:
        cp.start()

    targets = [packed[slots + t] for t in range(slots)]
    ranks = []
    for t in range(slots):
        rank = jnp.int32(0)
        for u in range(slots):
            ahead = targets[u] <= targets[t] if u < t else targets[u] < targets[t]
            if u != t:
                rank = rank + jnp.where(ahead, 1, 0)
        ranks.append(rank)
    before = jnp.int32(-1)
    for n in range(slots):
        slot, target = jnp.int32(0), jnp.int32(0)
        for t in range(slots):
            slot = jnp.where(ranks[t] == n, t, slot)
            target = jnp.where(ranks[t] == n, targets[t], target)
        order[n] = slot
        joins[n] = jnp.where(target == before, 1.0, 0.0)
        before = target
    for s in range(S * K):
        last, below = jnp.int32(0), jnp.int32(0)
        for t in range(slots):
            last = last + jnp.where(targets[t] <= s, 1, 0)
            below = below + jnp.where(targets[t] < s, 1, 0)
        upto[s] = jnp.maximum(last - 1, 0)
        has[s] = jnp.where(last > below, 1.0, 0.0)

    for cp in own_loads:
        cp.wait()
    pl.semaphore_wait(barrier, len(direct) + z_sides)
    if Z > 2:
        signal_sides(ready.at[0])

    step = R // STEPS
    tail = (STEPS - RELAYED) * step
    pieces = [(d, j) for j in range(RELAYED) for d in range(1, S)]
    tails = list(range(1, S))

    def begin(*copies):
        for cp in copies:
            cp.start()

    def part(held, d, j, c):
        sectors = pl.ds(lax.rem(ym + S - d, S) * K, K)
        rows = pl.ds(RELAYED * step, tail) if j == RELAYED else pl.ds(j * step, step)
        return held.at[sectors, rows, pl.ds(pl.multiple_of(c * Q, 128), Q)]

    def y_copy(d, j, source):
        ref = part(near, source, j, cm)
        return remote(ref, ref, g_send.at[0], g_recv.at[d - 1, j], y_peer(d))

    def y_far(d, source):
        ref = part(far, source, RELAYED, cm)
        return remote(ref, ref, g_send.at[1], e_recv.at[d - 1], y_peer(d))

    def x_copy(d, j):
        ref = part(near, d, j, cm)
        dst = part(far, d, j, cm)
        return remote(ref, dst, g_send.at[2], h_recv.at[d - 1, j], x_peer)

    def core_copy(d, j, n, c):
        ref = part((near, far)[n], d, j, c)
        return remote(ref, ref, g_send.at[3 + n], f_recv.at[n], core_peer)

    for d, j in pieces:
        begin(y_copy(d, j, 0))
    for d in tails:
        begin(y_copy(d, RELAYED, 0))
    for d in tails:
        begin(y_far(d, 0))

    depth_ids = lax.broadcasted_iota(jnp.int32, (1, R), 1)
    chunk = 4 if slots % 4 == 0 else slots

    def first(n_held, zh, g):
        held = (near, far)[n_held]
        for n in range(g * chunk, (g + 1) * chunk):
            t = order[n]
            source = packed[t]
            limit = jnp.where(t < packed[2 * slots], packed[2 * slots + 1 + source], 0)
            keep = jnp.where(depth_ids < limit, 1.0, 0.0).astype(BF16)
            lmat = lbuf[t, zh].reshape(M, R) * keep
            value = jnp.dot(lmat, held[source], preferred_element_type=F32).astype(BF16)
            half[n, zh, :, n_held * H : (n_held + 1) * H] = value

    def second(zh, w):
        for n in range(slots):
            total = lax.dot_general(
                half[n, zh],
                rbuf[order[n], w * H : (w + 1) * H],
                (((1,), (1,)), ((), ())),
                preferred_element_type=F32,
            )
            total = total.reshape(prod.shape[3:])
            if n > 0:
                total = total + prod[zh, w, n - 1] * joins[n]
            prod[zh, w, n] = total

    def core_send(zh, w):
        return remote(
            snd_c.at[zh, w], rcv_c.at[zh, w], r_send.at[0], c_recv.at[zh, w], core_peer
        )

    def spread(zh, w):
        @pl.loop(0, S * K, unroll=4)
        def _(s):
            y, k = s // K, s % K
            away = prod[zh, w, upto[s], co] * has[s]
            snd_c[zh, w, y, k] = away.astype(BF16).reshape(X, Z2, B, H)

        begin(core_send(zh, w))

    handled = []

    def relay_far(count):
        for d, j in pieces[len(handled) : len(handled) + count]:
            x_copy(d, j).wait_recv()
            begin(core_copy(d, j, 1, cm))
            handled.append((d, j))

    for n, (d, j) in enumerate(pieces):
        y_copy(d, j, d).wait_recv()
        begin(x_copy(d, j), core_copy(d, j, 0, cm))
        if n >= LAG:
            relay_far(1)
    for d in tails:
        y_copy(d, RELAYED, d).wait_recv()
        begin(core_copy(d, RELAYED, 0, cm))
        relay_far(1)
    if Z > 2:
        pl.semaphore_wait(ready.at[0], z_sides)
        if Z > 3:
            signal_sides(ready.at[1])
    relay_far(len(pieces))
    for d in tails:
        y_far(d, d).wait_recv()
        begin(core_copy(d, RELAYED, 1, cm))
    pltpu.make_async_copy(lbuf, lbuf, load_sem.at[3]).wait()
    pltpu.make_async_copy(rbuf, rbuf, load_sem.at[4]).wait()
    others = pl.ds(0, (S - 1) * K)

    def shares(held, rows):
        return held.at[others, rows, pl.ds(0, Q)]

    whole, most, rest = pl.ds(0, R), pl.ds(0, RELAYED * step), pl.ds(0, tail)

    def all_of(held, rows, ssem, rsem, peer):
        return remote(shares(held, rows), shares(held, rows), ssem, rsem, peer)

    def base(zh, w, y, k, x):
        s = y * K + k
        rows = pl.ds(pl.multiple_of(x * Z2 * B, Z2 * B), Z2 * B)
        own = prod[zh, w, upto[s], cm, rows, :] * has[s]
        return own.reshape(Z2, B, H) + rcv_c[zh, w, y, k, x].astype(F32)

    def a1_copy(zh, y):
        at = (zh, y)
        return remote(snd_a1.at[at], rcv_a1.at[at], r_send.at[1], ra1.at[at], x_peer)

    def b1_copy(zh, away, d):
        at = (zh, away, d - 1)
        return remote(snd_b1.at[at], rcv_b1.at[at], r_send.at[2], rb1.at[at], y_peer(d))

    def a2_copy(zh, d, k):
        at = (zh, d - 1, k)
        return remote(snd_a2.at[at], rcv_a2.at[at], r_send.at[3], ra2.at[at], y_peer(d))

    def b2_copy(zh, k):
        at = (zh, k)
        return remote(snd_b2.at[at], rcv_b2.at[at], r_send.at[4], rb2.at[at], x_peer)

    def z_copy(zh, w, k, i):
        z = zh * Z2 + i
        slot = lax.rem(zm - z - 1 + 2 * Z, Z)
        return remote(
            snd_z.at[zh, i, w, k],
            rcv_z.at[w, k, slot],
            z_send.at[zh, i],
            rz.at[w, k],
            dev(z, xm, cm, ym),
        )

    def stage_one_a(zh):
        core_send(zh, 0).wait_recv()
        for d in list(range(1, S)) + [0]:
            y = y_other(d)
            for k in range(K):
                snd_a1[zh, y, k] = base(zh, 0, y, k, xo).astype(BF16)
            begin(a1_copy(zh, y))

    def stage_one_b(zh):
        core_send(zh, 1).wait_recv()
        for away, x in ((0, xo), (1, xm)):
            for d in range(1, S):
                for k in range(K):
                    snd_b1[zh, away, d - 1, k] = base(zh, 1, y_other(d), k, x).astype(BF16)
                begin(b1_copy(zh, away, d))

    def stage_two_a(zh):
        for d in range(1, S):
            yo = y_other(d)
            a1_copy(zh, yo).wait_recv()
            for k in range(K):
                total = base(zh, 0, yo, k, xm) + rcv_a1[zh, yo, k].astype(F32)
                snd_a2[zh, d - 1, k] = total.astype(BF16)
                begin(a2_copy(zh, d, k))

    def stage_two_b(zh):
        for d in range(1, S):
            b1_copy(zh, 0, d).wait_recv()
        for k in range(K):
            total = base(zh, 1, ym, k, xo)
            for d in range(1, S):
                total = total + rcv_b1[zh, 0, d - 1, k].astype(F32)
            snd_b2[zh, k] = total.astype(BF16)
            begin(b2_copy(zh, k))

    def z_own(zh, w, k, i):
        s = ym * K + k
        rows = pl.ds(pl.multiple_of((xm * Z2 + i) * B, B), B)
        total = prod[zh, w, upto[s], cm, rows, :] * has[s]
        total = total + rcv_c[zh, w, ym, k, xm, i].astype(F32)
        if w == 0:
            total = total + rcv_a1[zh, ym, k, i].astype(F32)
            for d in range(1, S):
                total = total + rcv_a2[zh, d - 1, k, i].astype(F32)
        else:
            for d in range(1, S):
                total = total + rcv_b1[zh, 1, d - 1, k, i].astype(F32)
            total = total + rcv_b2[zh, k, i].astype(F32)
        return total

    def stage_three(zh):
        a1_copy(zh, ym).wait_recv()
        for d in range(1, S):
            b1_copy(zh, 1, d).wait_recv()
        for k in range(K):
            for w in range(2):
                if w == 0:
                    for d in range(1, S):
                        a2_copy(zh, d, k).wait_recv()
                else:
                    b2_copy(zh, k).wait_recv()
                for i in range(Z2):
                    @pl.when(zm != zh * Z2 + i)
                    def _():
                        snd_z[zh, i, w, k] = z_own(zh, w, k, i).astype(BF16)
                        begin(z_copy(zh, w, k, i))

    def first_all(n_held, zh):
        for g in range(slots // chunk):
            first(n_held, zh, g)

    all_of(near, whole, g_send.at[3], f_recv.at[0], core_peer).wait_recv()
    first_all(0, 0)
    all_of(far, whole, g_send.at[4], f_recv.at[1], core_peer).wait_recv()
    first_all(1, 0)
    second(0, 0)
    spread(0, 0)
    second(0, 1)
    spread(0, 1)
    stage_one_a(0)
    first_all(0, 1)
    stage_one_b(0)
    first_all(1, 1)
    second(1, 0)
    spread(1, 0)
    second(1, 1)
    spread(1, 1)
    stage_two_a(0)
    stage_two_b(0)
    stage_one_a(1)
    stage_one_b(1)
    for p in range(1, Z - 2):
        pl.semaphore_wait(ready.at[p], z_sides)
        if p + 1 < Z - 2:
            signal_sides(ready.at[p + 1])
    stage_three(0)
    stage_two_a(1)
    stage_two_b(1)
    stage_three(1)

    ids = term * B + lax.broadcasted_iota(jnp.int32, (B, H), 0)
    my_half, my_place = zm // Z2, lax.rem(zm, Z2)
    for k in range(K):
        used = ids < packed[2 * slots + 1 + ym * K + k]
        for w in range(2):
            total = z_own(my_half, w, k, my_place)
            got = rcv_z.at[w, k]
            remote(got, got, r_send.at[0], rz.at[w, k], core_peer).wait_recv()
            for n in range(Z - 1):
                total = total + rcv_z[w, k, n].astype(F32)
            out[k, :, w * H : (w + 1) * H] = jnp.where(used, total, 0.0)

    all_of(near, whole, g_send.at[0], f_recv.at[0], core_peer).wait_send()
    all_of(far, rest, g_send.at[1], f_recv.at[0], core_peer).wait_send()
    all_of(near, most, g_send.at[2], f_recv.at[0], core_peer).wait_send()
    all_of(near, whole, g_send.at[3], f_recv.at[0], core_peer).wait_send()
    all_of(far, whole, g_send.at[4], f_recv.at[0], core_peer).wait_send()
    for n, ref in enumerate((snd_c, snd_a1, snd_b1, snd_a2, snd_b2)):
        remote(ref, ref, r_send.at[n], f_recv.at[0], core_peer).wait_send()
    for zh in range(2):
        for i in range(Z2):
            @pl.when(zm != zh * Z2 + i)
            def _():
                ref = snd_z.at[zh, i]
                remote(ref, ref, z_send.at[zh, i], f_recv.at[0], core_peer).wait_send()


def local(mesh_sizes, wave, left, right, source, target, live, sector_rows):
    T, S = mesh_sizes
    X = 2
    Z = T // (2 * X)
    K, R, C = wave.shape
    B = R // T
    H, Q = C // 2, C // 4
    slots = left.shape[0]
    dims = (Z, X, S, K, B, C)
    left = left.reshape(slots, 2, Z // 2, X, 2, B, R)
    vm = pltpu.VMEM
    dma = pltpu.SemaphoreType.DMA
    Z2 = Z // 2
    share = (K, Z2, B, H)
    scratch = [
        vm((S * K, R, H), BF16),
        vm((S * K, R, H), BF16),
        vm((slots, 2, 2, X, Z2, B, R), BF16),
        vm((slots, C, C), BF16),
        vm((slots, 2, R // 2, C), BF16),
        vm((2, 2, slots, 2, X * Z2 * B, H), F32),
        vm((2, 2, S, K, X, Z2, B, H), BF16),
        vm((2, 2, S, K, X, Z2, B, H), BF16),
        vm((2, S) + share, BF16),
        vm((2, S) + share, BF16),
        vm((2, 2, S - 1) + share, BF16),
        vm((2, 2, S - 1) + share, BF16),
        vm((2, S - 1) + share, BF16),
        vm((2, S - 1) + share, BF16),
        vm((2,) + share, BF16),
        vm((2,) + share, BF16),
        vm((2, Z2, 2, K, B, H), BF16),
        vm((2, K, Z - 1, B, H), BF16),
        pltpu.SMEM((slots,), jnp.int32),
        pltpu.SMEM((slots,), F32),
        pltpu.SMEM((S * K,), jnp.int32),
        pltpu.SMEM((S * K,), F32),
        dma((5,)),
        pltpu.SemaphoreType.REGULAR((max(Z - 2, 1),)),
        dma((5,)),
        dma((S - 1, RELAYED + 1)),
        dma((S - 1,)),
        dma((S - 1, RELAYED)),
        dma((2,)),
        dma((5,)),
        dma((2, Z2)),
        dma((2, 2)),
        dma((2, S)),
        dma((2, 2, S - 1)),
        dma((2, S - 1, K)),
        dma((2, K)),
        dma((2, K)),
    ]
    any_spec = pl.BlockSpec(memory_space=pl.ANY)
    smem = pl.BlockSpec(memory_space=pltpu.SMEM)
    return pl.pallas_call(
        functools.partial(kernel, dims),
        out_shape=jax.ShapeDtypeStruct((K, B, C), F32),
        in_specs=[any_spec] * 3 + [smem],
        out_specs=pl.BlockSpec(memory_space=pltpu.VMEM),
        scratch_shapes=scratch,
        compiler_params=pltpu.CompilerParams(
            collective_id=0, has_side_effects=True, vmem_limit_bytes=54784 * 1024
        ),
    )(wave, left, right, jnp.concatenate([source, target, live, sector_rows]))


def solution(mesh):
    in_specs = (
        P("sector", None, None),
        P(("term", "sector"), None, None),
        P(("term", "sector"), None, None),
        P(("term", "sector")),
        P(("term", "sector")),
        P(("term", "sector")),
        P(),
    )
    out_specs = P("sector", "term", None)
    sizes = (mesh.shape["term"], mesh.shape["sector"])
    return jax.shard_map(
        functools.partial(local, sizes),
        mesh=mesh,
        in_specs=in_specs,
        out_specs=out_specs,
        check_vma=False,
    )
```
